32 devices in a mesh: row: 4 (over z), col: 4 (over y, core), depth: 2 (over x).
Axes of the slice: x: 2, y: 2, z: 4, core: 2. Of those that a mesh axis runs over, the one named last changes fastest.
Arguments:
- grad_out: bfloat16 [2, 2048, 8192], P('depth', 'col', 'row'), may hold values from -0.09375 to 0.09375
- inputs: bfloat16 [2, 2048, 8192], P('depth', 'row', 'col'), may hold values from -6 to 6
Outputs:
- grad_weight: bfloat16 [8192, 8192], P(('row', 'depth'), 'col')
The draws below stay inside these ranges and needn't reach their ends.
All inputs are finite; a program needn't handle non-finite values.
Results may differ from the reference program's by a relative error of at most 0.001.
Values may be sent and summed in bfloat16 or wider, within the bound.
A program may use at most 128 MiB of HBM per device.

```python
import jax
import jax.numpy as jnp

D = 8192
LAYER_TOK = 2048
MICRO = 2
TOKENS = 4096


def strengthened(array, stream_key, source, target, parts, factor):
    owner, partner = [(jnp.arange(array.shape[dim]) // (array.shape[dim] // parts)).reshape([-1 if axis == dim else 1 for axis in range(array.ndim)]) for dim in (source, target)]
    chosen = jax.random.permutation(stream_key, parts)[partner]
    strong = (owner == chosen) | (owner == (partner + parts // 2) % parts)
    return jnp.where(strong, factor * array, array)


def block_scale(stream_key, dims, split, smallest, largest):
    gain, own = 1.0, jax.random.fold_in(stream_key, 6)
    for axis_at, blocks in split:
        steps = jnp.exp(jax.random.uniform(jax.random.fold_in(own, axis_at), (blocks,), jnp.float32, smallest / len(split), largest / len(split)))
        gain = gain * jnp.repeat(steps, dims[axis_at] // blocks).reshape([-1 if axis == axis_at else 1 for axis in range(len(dims))])
    return gain


def scatter_about(stream_key, extent, deviation, limit, shards=(), dtype=jnp.bfloat16):
    entries = jax.random.normal(stream_key, extent, jnp.float32) * deviation
    if len(shards) > 0:
        entries = block_scale(stream_key, extent, shards, -0.22, 0.18) * entries
    return jnp.clip(entries, min=-limit, max=limit).astype(dtype)


def gaussian_with(own_key, extent, scale, limit, pieces, heavy, dtype=jnp.bfloat16):
    drawn = scale * jax.random.normal(own_key, extent, jnp.float32)
    if pieces:
        drawn = drawn * block_scale(own_key, extent, pieces, -0.22, 0.18)
    return jnp.clip(strengthened(drawn, jax.random.fold_in(own_key, 3), *heavy), -limit, limit).astype(dtype)


def setup_inputs(seed: int = 0) -> dict:
    key_of = jax.random.split(jax.random.key(seed), 3)
    return {
        "grad_out": gaussian_with(key_of[0], (MICRO, LAYER_TOK, D), (1.0 / TOKENS ** 0.5), 0.09375, ((0, 2), (1, 4), (2, 4)), (0, 2, 2, 2.0)),
        "inputs": scatter_about(key_of[1], (MICRO, LAYER_TOK, D), 1.0, 6.0, ((0, 2), (1, 4), (2, 4))),
    }


def reference(grad_out, inputs):
    width = grad_out.shape[2]
    left = grad_out.reshape(-1, width)
    right = inputs.reshape(-1, width)
    result = jnp.dot(left.T, right, preferred_element_type=jnp.float32)
    return result.astype(jnp.bfloat16)
```

```python
import functools
import math

import jax
import jax.numpy as jnp
from jax import lax
from jax.experimental import pallas as pl
from jax.experimental.pallas import tpu as pltpu
from jax.sharding import PartitionSpec as P

MESH = pl.DeviceIdType.MESH


def kernel(nr, nc, nd, Q, VQ, go_ref, in_ref, out_ref, abuf, at, bbuf, acc, loc_sem, ra, rb, ss):
    r, c, d = lax.axis_index("row"), lax.axis_index("col"), lax.axis_index("depth")
    ta, fh = abuf.shape[2], abuf.shape[3]
    tb, gw = bbuf.shape[2], bbuf.shape[3]
    cb = tb // Q
    has_up, has_dn = r < nr - 1, r > 0
    pending = []

    load_b = pltpu.make_async_copy(in_ref.at[0], bbuf.at[d, r], loc_sem.at[0])
    load_a = pltpu.make_async_copy(
        go_ref.at[0, :, pl.ds(pl.multiple_of(d * fh, 128), fh)], abuf.at[d, c], loc_sem.at[1]
    )
    load_b.start()
    load_a.start()

    def send(src, dst, recv_sem, device, cond=None):
        copy = pltpu.make_async_remote_copy(
            src_ref=src, dst_ref=dst, send_sem=ss.at[len(pending)], recv_sem=recv_sem,
            device_id=device, device_id_type=MESH,
        )
        pending.append((cond, copy))
        if cond is None:
            copy.start()
        else:
            pl.when(cond)(copy.start)

    def arrived(ref, sem):
        pltpu.make_async_copy(ref, ref, sem).wait()

    def b_chunk(m, b, q):
        return bbuf.at[m, b, pl.ds(q * cb, cb)]

    barrier = pltpu.get_barrier_semaphore()

    @pl.when(has_up)
    def _():
        pl.semaphore_signal(barrier, inc=1, device_id={"row": r + 1}, device_id_type=MESH)

    @pl.when(has_dn)
    def _():
        pl.semaphore_signal(barrier, inc=1, device_id={"row": r - 1}, device_id_type=MESH)

    for k in range(1, nd):
        pl.semaphore_signal(barrier, inc=1, device_id={"depth": lax.rem(d + k, nd)}, device_id_type=MESH)
    for k in range(1, nc):
        pl.semaphore_signal(barrier, inc=1, device_id={"col": lax.rem(c + k, nc)}, device_id_type=MESH)
    neighbours = jnp.where(has_up, 1, 0) + jnp.where(has_dn, 1, 0)
    pl.semaphore_wait(barrier, nd - 1 + nc - 1 + neighbours)

    peers = [lax.rem(d + k, nd) for k in range(1, nd)]

    def to_up(m, b, q, cond):
        send(b_chunk(m, b, q), b_chunk(m, b, q), rb.at[m, b, q], {"row": jnp.minimum(r + 1, nr - 1)}, cond)

    def to_dn(m, b, q, cond):
        send(b_chunk(m, b, q), b_chunk(m, b, q), rb.at[m, b, q], {"row": jnp.maximum(r - 1, 0)}, cond)

    def to_depth(b, q, cond=None):
        for p in peers:
            send(b_chunk(d, b, q), b_chunk(d, b, q), rb.at[d, b, q], {"depth": p}, cond)

    def a_to_col(m):
        for k in range(1, nc):
            send(abuf.at[m, c], abuf.at[m, c], ra.at[m, c], {"col": lax.rem(c + k, nc)})

    for p in peers:
        src = go_ref.at[0, :, pl.ds(pl.multiple_of(p * fh, 128), fh)]
        send(src, abuf.at[d, c], ra.at[d, c], {"depth": p})
    load_b.wait()
    for q in range(Q):
        to_up(d, r, q, has_up)
        to_dn(d, r, q, has_dn)
        to_depth(r, q)
    load_a.wait()
    a_to_col(d)

    def transpose_a(m):
        def blk(cc, _):
            def tile(j, _):
                j0 = pl.multiple_of(j * 128, 128)
                at[m, pl.ds(j0, 128), pl.ds(pl.multiple_of(cc * ta, 128), ta)] = abuf[
                    m, cc, :, pl.ds(j0, 128)
                ].T
                return 0

            return lax.fori_loop(0, fh // 128, tile, 0)

        lax.fori_loop(0, nc, blk, 0)

    tm, tn = min(512, fh), min(512, gw)

    def multiply(m, b, q0, q1, first=False):
        rows = (q1 - q0) * cb

        def tile(i, _):
            i0 = pl.multiple_of((i // (gw // tn)) * tm, tm)
            j0 = pl.multiple_of(lax.rem(i, gw // tn) * tn, tn)
            left = at[m, pl.ds(i0, tm), pl.ds(pl.multiple_of(b * tb + q0 * cb, 128), rows)]
            right = bbuf[m, b, pl.ds(q0 * cb, rows), pl.ds(j0, tn)]
            part = jnp.dot(left, right, preferred_element_type=jnp.float32)
            if first:
                acc[pl.ds(i0, tm), pl.ds(j0, tn)] = part
            else:
                acc[pl.ds(i0, tm), pl.ds(j0, tn)] += part
            return 0

        lax.fori_loop(0, (fh // tm) * (gw // tn), tile, 0)

    def both_sides(s, fn):
        def side(i, _):
            b = r + s * (2 * i - 1)

            @pl.when(jnp.logical_and(b >= 0, b < nr))
            def _():
                fn(b)

            return 0

        lax.fori_loop(0, 2, side, 0)

    def wait_a(m):
        for k in range(1, nc):
            cc = lax.rem(c + k, nc)
            arrived(abuf.at[m, cc], ra.at[m, cc])

    def forward_a():
        for p in peers:
            arrived(abuf.at[p, c], ra.at[p, c])
            a_to_col(p)

    relay_at = max(1, nr - 2)
    for s in range(1, nr):
        lo, hi = r - s, r + s
        for q in range(Q):
            pl.when(lo >= 0)(lambda: arrived(b_chunk(d, lo, q), rb.at[d, lo, q]))
            to_up(d, lo, q, jnp.logical_and(lo >= 0, has_up))
            if not (s == 1 and q < VQ):
                to_depth(lo, q, lo >= 0)
            pl.when(hi < nr)(lambda: arrived(b_chunk(d, hi, q), rb.at[d, hi, q]))
            to_dn(d, hi, q, jnp.logical_and(hi < nr, has_dn))
            if not (s == 1 and q < VQ):
                to_depth(hi, q, hi < nr)
            if s == 1 and q == (Q - 1) // 2:
                forward_a()
        if s == relay_at:
            for p in peers:
                for q in range(Q):
                    arrived(b_chunk(p, r, q), rb.at[p, r, q])
                    if q < VQ:
                        to_up(p, r, q, has_up)
                        to_dn(p, r, q, has_dn)
        if s == 1:
            wait_a(d)
            transpose_a(d)
            multiply(d, r, 0, Q, first=True)
        both_sides(s, lambda b: multiply(d, b, 0, Q))
        if s == relay_at:
            for p in peers:
                wait_a(p)
                transpose_a(p)
                multiply(p, r, 0, Q)

    def take(p, b, q0, q1):
        for q in range(q0, q1):
            arrived(b_chunk(p, b, q), rb.at[p, b, q])
        multiply(p, b, q0, q1)

    half = max(1, Q // 2)
    for s in list(range(2, nr)) + [1]:
        for p in peers:
            for q0 in range(0, Q, half):
                both_sides(s, lambda b: take(p, b, q0, q0 + half))

    def store(i, _):
        i0 = pl.multiple_of(i * 128, 128)
        out_ref[pl.ds(i0, 128), :] = acc[pl.ds(i0, 128), :].astype(out_ref.dtype)
        return 0

    lax.fori_loop(0, fh // 128, store, 0)
    for cond, copy in pending:
        if cond is None:
            copy.wait_send()
        else:
            pl.when(cond)(copy.wait_send)


def count_sends(nr, nc, nd, Q):
    return (nd - 1) + nd * (nc - 1) + 2 * nr * Q * nd + 2 * (nd - 1) * Q


MIB = 2**20


def split_kernel(
    nr, nc, J, QA, QX, go_ref, in_ref, out_ref,
    abuf, at, bbuf, acc, stage, ls, ra, rb, ro, sb, sx, sa, so,
):
    r, c, d = lax.axis_index("row"), lax.axis_index("col"), lax.axis_index("depth")
    e = 1 - d
    core = lax.rem(c, 2)
    sib = c + 1 - 2 * core
    others = [lax.rem(c + 2 * k, nc) for k in range(1, nc // 2)]
    nd = 2
    ta, f = abuf.shape[2], abuf.shape[3]
    w = bbuf.shape[3]
    tb = bbuf.shape[2] // nr
    fh, gh = f // nd, J * w
    ca = ta // QA
    has_up, has_dn = r < nr - 1, r > 0
    up, dn = {"row": jnp.minimum(r + 1, nr - 1)}, {"row": jnp.maximum(r - 1, 0)}
    peer, twin = {"depth": e}, {"col": sib}

    def cols(half, j):
        return pl.ds(pl.multiple_of(half * gh + j * w, 128), w)

    def b_piece(m, b, j):
        return bbuf.at[m, j, pl.ds(pl.multiple_of(b * tb, 128), tb)]

    def a_piece(m, cc, q):
        return abuf.at[m, cc, pl.ds(q * ca, ca)]

    def loop(n, fn):
        lax.fori_loop(0, n, lambda i, _: (fn(i), 0)[1], 0)

    def arrived(ref, sem):
        pltpu.make_async_copy(ref, ref, sem).wait()

    def send(src, dst, send_sem, recv_sem, device):
        pltpu.make_async_remote_copy(
            src_ref=src, dst_ref=dst, send_sem=send_sem, recv_sem=recv_sem,
            device_id=device, device_id_type=MESH,
        ).start()

    loop(J, lambda j: pltpu.make_async_copy(in_ref.at[0, :, cols(d, j)], b_piece(d, r, j), ls.at[j]).start())
    load_a = pltpu.make_async_copy(go_ref.at[0], abuf.at[d, c], ls.at[J])
    load_a.start()

    barrier = pltpu.get_barrier_semaphore()

    def greet(device):
        pl.semaphore_signal(barrier, inc=1, device_id=device, device_id_type=MESH)

    pl.when(has_up)(lambda: greet(up))
    pl.when(has_dn)(lambda: greet(dn))
    greet(peer)
    greet(twin)
    for o in others:
        greet({"col": o})
    pl.semaphore_wait(
        barrier, 2 + len(others) + jnp.where(has_up, 1, 0) + jnp.where(has_dn, 1, 0)
    )

    def b_up(m, b, j):
        send(b_piece(m, b, j), b_piece(m, b, j), sb.at[0, m, b, j], rb.at[m, b, j], up)

    def b_dn(m, b, j):
        send(b_piece(m, b, j), b_piece(m, b, j), sb.at[1, m, b, j], rb.at[m, b, j], dn)

    def b_both(m, j):
        pl.when(has_up)(lambda: b_up(m, r, j))
        pl.when(has_dn)(lambda: b_dn(m, r, j))

    def b_wait(m, b, j):
        arrived(b_piece(m, b, j), rb.at[m, b, j])

    def a_send(kind, m, cc, q, device):
        send(a_piece(m, cc, q), a_piece(m, cc, q), sa.at[kind, m, cc, q], ra.at[m, cc, q], device)

    def a_wait(m, cc, q):
        arrived(a_piece(m, cc, q), ra.at[m, cc, q])

    TWIN, PEER, OTHER = 0, 1, 2

    def first(j):
        send(in_ref.at[0, :, cols(e, j)], b_piece(d, r, j), sx.at[j], rb.at[d, r, j], peer)
        pltpu.make_async_copy(in_ref.at[0, :, cols(d, j)], b_piece(d, r, j), ls.at[j]).wait()
        b_both(d, j)

    loop(J, first)
    load_a.wait()

    def own_a(q):
        a_send(PEER, d, c, q, peer)
        for k, o in enumerate(others):
            a_send(OTHER + k, d, c, q, {"col": o})
        a_send(TWIN, d, c, q, twin)

    loop(QA, own_a)

    def second(j):
        b_wait(e, r, j)
        b_both(e, j)

    loop(J, second)

    def pass_on(s, j, wait=True, go=True):
        lo, hi = r - s, r + s
        for m in (d, e):
            @pl.when(jnp.logical_and(lo >= 0, has_up))
            def _():
                if wait:
                    b_wait(m, lo, j)
                if go:
                    b_up(m, lo, j)

            @pl.when(jnp.logical_and(hi < nr, has_dn))
            def _():
                if wait:
                    b_wait(m, hi, j)
                if go:
                    b_dn(m, hi, j)

    LEAD = min(2, J)

    def near(j):
        pl.when(j < J)(lambda: pass_on(1, j, wait=False))

    def far(j):
        @pl.when(j < J)
        def _():
            for s in range(2, nr):
                pass_on(s, j)

    def from_other(q):
        for o in others:
            a_wait(d, o, q)
            a_send(TWIN, d, o, q, twin)
            if q < QX:
                a_send(PEER, d, o, q, peer)

    def from_peer(q):
        a_wait(e, c, q)
        if q >= QX:
            for k, o in enumerate(others):
                a_send(OTHER + k, e, c, q, {"col": o})
        a_send(TWIN, e, c, q, twin)

    def from_corner(q):
        for o in others:
            a_wait(e, o, q)
            a_send(TWIN, e, o, q, twin)

    def from_twin(m):
        for o in [sib] + [lax.rem(sib + 2 * k, nc) for k in range(1, nc // 2)]:
            for q in range(QA):
                a_wait(m, o, q)

    def transpose_a(m):
        def blk(cc):
            def tile(j):
                j0 = pl.multiple_of(j * 128, 128)
                at[m, pl.ds(j0, 128), pl.ds(pl.multiple_of(cc * ta, 128), ta)] = abuf[
                    m, cc, :, pl.ds(j0, 128)
                ].T

            loop(f // 128, tile)

        loop(nc, blk)

    tm = min(512, fh)

    def left(m, b, i):
        return at[m, pl.ds(pl.multiple_of(i * tm, tm), tm), pl.ds(pl.multiple_of(b * tb, 128), tb)]

    def multiply_pairs(m, b, start=False):
        def tile(n):
            i, j = n // (J // 2), 2 * lax.rem(n, J // 2)
            rows = pl.ds(pl.multiple_of(i * tm, tm), tm)
            right = jnp.concatenate([b_piece(m, b, j)[...], b_piece(m, b, j + 1)[...]], axis=1)
            part = jnp.dot(left(m, b, i), right, preferred_element_type=jnp.float32)
            for k in range(2):
                if start:
                    acc[j + k, rows] = part[:, k * w : (k + 1) * w]
                else:
                    acc[j + k, rows] += part[:, k * w : (k + 1) * w]

        loop((f // tm) * (J // 2), tile)

    def multiply(m, b, j):
        def tile(i):
            rows = pl.ds(pl.multiple_of(i * tm, tm), tm)
            acc[j, rows] += jnp.dot(left(m, b, i), b_piece(m, b, j)[...], preferred_element_type=jnp.float32)

        loop(f // tm, tile)

    def both_sides(s, fn):
        def side(i):
            b = r + s * (2 * i - 1)
            pl.when(jnp.logical_and(b >= 0, b < nr))(lambda: fn(b))

        loop(2, side)

    def not_passed(b):
        return jnp.logical_or(
            jnp.logical_and(b < r, jnp.logical_not(has_up)),
            jnp.logical_and(b > r, jnp.logical_not(has_dn)),
        )

    def b_here(m, b, j):
        pl.when(not_passed(b))(lambda: b_wait(m, b, j))

    loop(LEAD, lambda j: pass_on(1, j))
    for q in range(QA - 1):
        from_other(q)
    from_peer(0)
    from_other(QA - 1)
    from_peer(1)
    from_twin(d)
    loop(J - LEAD, lambda j: pass_on(1, LEAD + j, go=False))
    transpose_a(d)
    far(0)
    near(LEAD)
    multiply_pairs(d, r, start=True)

    def near_block(b):
        loop(J, lambda j: b_here(d, b, j))
        multiply_pairs(d, b)

    both_sides(1, near_block)
    from_peer(2)
    from_corner(1)
    far(1)
    near(LEAD + 1)
    for q in range(3, QA):
        from_peer(q)
        from_corner(q - 1)
    far(2)
    near(LEAD + 2)
    from_corner(QA - 1)
    from_corner(0)
    far(3)
    near(LEAD + 3)
    from_twin(e)
    transpose_a(e)

    def column(j):
        far(j + 4)
        near(j + LEAD + 4)
        multiply(e, r, j)

        def one(s, m, b):
            b_here(m, b, j)
            multiply(m, b, j)

        both_sides(1, lambda b: one(1, e, b))
        for s in range(2, nr):
            for m in (d, e):
                both_sides(s, lambda b: one(s, m, b))

        def rows(i):
            i0 = pl.multiple_of(i * 128, 128)
            stage[j, pl.ds(i0, 128), :] = acc[j, pl.ds(pl.multiple_of(e * fh, 128) + i0, 128)].astype(jnp.bfloat16)

        loop(fh // 128, rows)

        def mine(i):
            i0 = pl.multiple_of(i * 128, 128)
            out_ref[pl.ds(i0, 128), cols(d, j)] = acc[j, pl.ds(pl.multiple_of(d * fh, 128) + i0, 128)].astype(jnp.bfloat16)

        loop(fh // 128, mine)
        send(stage.at[j], out_ref.at[:, cols(d, j)], so.at[j], ro.at[j], peer)

    loop(J, column)

    def drain(j):
        arrived(out_ref.at[:, cols(e, j)], ro.at[j])
        arrived(stage.at[j], so.at[j])
        arrived(b_piece(d, r, j), sx.at[j])
        for m in range(nd):
            def one(b):
                pl.when(jnp.logical_and(has_up, b <= r))(lambda: arrived(b_piece(m, b, j), sb.at[0, m, b, j]))
                pl.when(jnp.logical_and(has_dn, b >= r))(lambda: arrived(b_piece(m, b, j), sb.at[1, m, b, j]))

            loop(nr, one)

    loop(J, drain)

    def drain_a(q):
        def sent(kind, m, cc):
            arrived(a_piece(m, cc, q), sa.at[kind, m, cc, q])

        for m in range(nd):
            for cc in [c] + others:
                sent(TWIN, m, cc)
        sent(PEER, d, c)
        for k in range(len(others)):
            sent(OTHER + k, d, c)
        if q < QX:
            for o in others:
                sent(PEER, d, o)
        else:
            for k in range(len(others)):
                sent(OTHER + k, e, c)

    for q in range(QA):
        drain_a(q)


def split_plan(nr, nc, nd, ta, tb, f, gw):
    w = 128
    if nd != 2 or nc % 2 or nc < 4 or nr < 2 or gw % (nd * 2 * w) or ta % 512 or tb % 128 or f % 1024:
        return None
    J = gw // (nd * w)
    shapes = [
        ((nd, nc, ta, f), jnp.bfloat16),
        ((nd, f, ta * nc), jnp.bfloat16),
        ((nd, J, tb * nr, w), jnp.bfloat16),
        ((J, f, w), jnp.float32),
        ((J, f // nd, w), jnp.bfloat16),
    ]
    size = sum(math.prod(s) * jnp.dtype(t).itemsize for s, t in shapes)
    return (J, shapes) if size <= 52 * MIB else None


def split_body(nr, nc, nd, plan, grad_out, inputs):
    J, shapes = plan
    _, ta, f = grad_out.shape
    gw = inputs.shape[2]
    QA, QX = 4, 1
    return pl.pallas_call(
        functools.partial(split_kernel, nr, nc, J, QA, QX),
        out_shape=pltpu.VMEM((f // nd, gw), jnp.bfloat16),
        in_specs=[pl.BlockSpec(memory_space=pl.ANY)] * 2,
        out_specs=pl.BlockSpec(memory_space=pltpu.VMEM),
        scratch_shapes=[pltpu.VMEM(s, t) for s, t in shapes] + [
            pltpu.SemaphoreType.DMA((J + 1,)),
            pltpu.SemaphoreType.DMA((nd, nc, QA)),
            pltpu.SemaphoreType.DMA((nd, nr, J)),
            pltpu.SemaphoreType.DMA((J,)),
            pltpu.SemaphoreType.DMA((2, nd, nr, J)),
            pltpu.SemaphoreType.DMA((J,)),
            pltpu.SemaphoreType.DMA((1 + nc // 2, nd, nc, QA)),
            pltpu.SemaphoreType.DMA((J,)),
        ],
        compiler_params=pltpu.CompilerParams(
            collective_id=1, has_side_effects=True, vmem_limit_bytes=58 * MIB
        ),
    )(grad_out, inputs)


def body(nr, nc, nd, grad_out, inputs):
    _, ta, f = grad_out.shape
    _, tb, gw = inputs.shape
    fh = f // nd
    Q = max(1, min(4, 32 // (nd * nr)))
    VQ = 3 * Q // 4
    tokens = tb * nr
    plan = split_plan(nr, nc, nd, ta, tb, f, gw)
    if plan is not None:
        return split_body(nr, nc, nd, plan, grad_out, inputs)
    return pl.pallas_call(
        functools.partial(kernel, nr, nc, nd, Q, VQ),
        out_shape=pltpu.VMEM((fh, gw), jnp.bfloat16),
        in_specs=[pl.BlockSpec(memory_space=pl.ANY)] * 2,
        out_specs=pl.BlockSpec(memory_space=pltpu.VMEM),
        scratch_shapes=[
            pltpu.VMEM((nd, nc, ta, fh), jnp.bfloat16),
            pltpu.VMEM((nd, fh, tokens), jnp.bfloat16),
            pltpu.VMEM((nd, nr, tb, gw), jnp.bfloat16),
            pltpu.VMEM((fh, gw), jnp.float32),
            pltpu.SemaphoreType.DMA((2,)),
            pltpu.SemaphoreType.DMA((nd, nc)),
            pltpu.SemaphoreType.DMA((nd, nr, Q)),
            pltpu.SemaphoreType.DMA((count_sends(nr, nc, nd, Q),)),
        ],
        compiler_params=pltpu.CompilerParams(
            collective_id=0, has_side_effects=True, vmem_limit_bytes=52 * 2**20
        ),
    )(grad_out, inputs)


def solution(mesh):
    return jax.shard_map(
        functools.partial(body, mesh.shape["row"], mesh.shape["col"], mesh.shape["depth"]),
        mesh=mesh,
        in_specs=(P("depth", "col", "row"), P("depth", "row", "col")),
        out_specs=P(("row", "depth"), "col"),
        check_vma=False,
    )
```

```python
import functools
import math

import jax
import jax.numpy as jnp
from jax import lax
from jax.experimental import pallas as pl
from jax.experimental.pallas import tpu as pltpu
from jax.sharding import PartitionSpec as P

MESH = pl.DeviceIdType.MESH


def kernel(nr, nc, nd, Q, VQ, go_ref, in_ref, out_ref, abuf, at, bbuf, acc, loc_sem, ra, rb, ss):
    r, c, d = lax.axis_index("row"), lax.axis_index("col"), lax.axis_index("depth")
    ta, fh = abuf.shape[2], abuf.shape[3]
    tb, gw = bbuf.shape[2], bbuf.shape[3]
    cb = tb // Q
    has_up, has_dn = r < nr - 1, r > 0
    pending = []

    load_b = pltpu.make_async_copy(in_ref.at[0], bbuf.at[d, r], loc_sem.at[0])
    load_a = pltpu.make_async_copy(
        go_ref.at[0, :, pl.ds(pl.multiple_of(d * fh, 128), fh)], abuf.at[d, c], loc_sem.at[1]
    )
    load_b.start()
    load_a.start()

    def send(src, dst, recv_sem, device, cond=None):
        copy = pltpu.make_async_remote_copy(
            src_ref=src, dst_ref=dst, send_sem=ss.at[len(pending)], recv_sem=recv_sem,
            device_id=device, device_id_type=MESH,
        )
        pending.append((cond, copy))
        if cond is None:
            copy.start()
        else:
            pl.when(cond)(copy.start)

    def arrived(ref, sem):
        pltpu.make_async_copy(ref, ref, sem).wait()

    def b_chunk(m, b, q):
        return bbuf.at[m, b, pl.ds(q * cb, cb)]

    barrier = pltpu.get_barrier_semaphore()

    @pl.when(has_up)
    def _():
        pl.semaphore_signal(barrier, inc=1, device_id={"row": r + 1}, device_id_type=MESH)

    @pl.when(has_dn)
    def _():
        pl.semaphore_signal(barrier, inc=1, device_id={"row": r - 1}, device_id_type=MESH)

    for k in range(1, nd):
        pl.semaphore_signal(barrier, inc=1, device_id={"depth": lax.rem(d + k, nd)}, device_id_type=MESH)
    for k in range(1, nc):
        pl.semaphore_signal(barrier, inc=1, device_id={"col": lax.rem(c + k, nc)}, device_id_type=MESH)
    neighbours = jnp.where(has_up, 1, 0) + jnp.where(has_dn, 1, 0)
    pl.semaphore_wait(barrier, nd - 1 + nc - 1 + neighbours)

    peers = [lax.rem(d + k, nd) for k in range(1, nd)]

    def to_up(m, b, q, cond):
        send(b_chunk(m, b, q), b_chunk(m, b, q), rb.at[m, b, q], {"row": jnp.minimum(r + 1, nr - 1)}, cond)

    def to_dn(m, b, q, cond):
        send(b_chunk(m, b, q), b_chunk(m, b, q), rb.at[m, b, q], {"row": jnp.maximum(r - 1, 0)}, cond)

    def to_depth(b, q, cond=None):
        for p in peers:
            send(b_chunk(d, b, q), b_chunk(d, b, q), rb.at[d, b, q], {"depth": p}, cond)

    def a_to_col(m):
        for k in range(1, nc):
            send(abuf.at[m, c], abuf.at[m, c], ra.at[m, c], {"col": lax.rem(c + k, nc)})

    for p in peers:
        src = go_ref.at[0, :, pl.ds(pl.multiple_of(p * fh, 128), fh)]
        send(src, abuf.at[d, c], ra.at[d, c], {"depth": p})
    load_b.wait()
    for q in range(Q):
        to_up(d, r, q, has_up)
        to_dn(d, r, q, has_dn)
        to_depth(r, q)
    load_a.wait()
    a_to_col(d)

    def transpose_a(m):
        def blk(cc, _):
            def tile(j, _):
                j0 = pl.multiple_of(j * 128, 128)
                at[m, pl.ds(j0, 128), pl.ds(pl.multiple_of(cc * ta, 128), ta)] = abuf[
                    m, cc, :, pl.ds(j0, 128)
                ].T
                return 0

            return lax.fori_loop(0, fh // 128, tile, 0)

        lax.fori_loop(0, nc, blk, 0)

    tm, tn = min(512, fh), min(512, gw)

    def multiply(m, b, q0, q1, first=False):
        rows = (q1 - q0) * cb

        def tile(i, _):
            i0 = pl.multiple_of((i // (gw // tn)) * tm, tm)
            j0 = pl.multiple_of(lax.rem(i, gw // tn) * tn, tn)
            left = at[m, pl.ds(i0, tm), pl.ds(pl.multiple_of(b * tb + q0 * cb, 128), rows)]
            right = bbuf[m, b, pl.ds(q0 * cb, rows), pl.ds(j0, tn)]
            part = jnp.dot(left, right, preferred_element_type=jnp.float32)
            if first:
                acc[pl.ds(i0, tm), pl.ds(j0, tn)] = part
            else:
                acc[pl.ds(i0, tm), pl.ds(j0, tn)] += part
            return 0

        lax.fori_loop(0, (fh // tm) * (gw // tn), tile, 0)

    def both_sides(s, fn):
        def side(i, _):
            b = r + s * (2 * i - 1)

            @pl.when(jnp.logical_and(b >= 0, b < nr))
            def _():
                fn(b)

            return 0

        lax.fori_loop(0, 2, side, 0)

    def wait_a(m):
        for k in range(1, nc):
            cc = lax.rem(c + k, nc)
            arrived(abuf.at[m, cc], ra.at[m, cc])

    def forward_a():
        for p in peers:
            arrived(abuf.at[p, c], ra.at[p, c])
            a_to_col(p)

    relay_at = max(1, nr - 2)
    for s in range(1, nr):
        lo, hi = r - s, r + s
        for q in range(Q):
            pl.when(lo >= 0)(lambda: arrived(b_chunk(d, lo, q), rb.at[d, lo, q]))
            to_up(d, lo, q, jnp.logical_and(lo >= 0, has_up))
            if not (s == 1 and q < VQ):
                to_depth(lo, q, lo >= 0)
            pl.when(hi < nr)(lambda: arrived(b_chunk(d, hi, q), rb.at[d, hi, q]))
            to_dn(d, hi, q, jnp.logical_and(hi < nr, has_dn))
            if not (s == 1 and q < VQ):
                to_depth(hi, q, hi < nr)
            if s == 1 and q == (Q - 1) // 2:
                forward_a()
        if s == relay_at:
            for p in peers:
                for q in range(Q):
                    arrived(b_chunk(p, r, q), rb.at[p, r, q])
                    if q < VQ:
                        to_up(p, r, q, has_up)
                        to_dn(p, r, q, has_dn)
        if s == 1:
            wait_a(d)
            transpose_a(d)
            multiply(d, r, 0, Q, first=True)
        both_sides(s, lambda b: multiply(d, b, 0, Q))
        if s == relay_at:
            for p in peers:
                wait_a(p)
                transpose_a(p)
                multiply(p, r, 0, Q)

    def take(p, b, q0, q1):
        for q in range(q0, q1):
            arrived(b_chunk(p, b, q), rb.at[p, b, q])
        multiply(p, b, q0, q1)

    half = max(1, Q // 2)
    for s in list(range(2, nr)) + [1]:
        for p in peers:
            for q0 in range(0, Q, half):
                both_sides(s, lambda b: take(p, b, q0, q0 + half))

    def store(i, _):
        i0 = pl.multiple_of(i * 128, 128)
        out_ref[pl.ds(i0, 128), :] = acc[pl.ds(i0, 128), :].astype(out_ref.dtype)
        return 0

    lax.fori_loop(0, fh // 128, store, 0)
    for cond, copy in pending:
        if cond is None:
            copy.wait_send()
        else:
            pl.when(cond)(copy.wait_send)


def count_sends(nr, nc, nd, Q):
    return (nd - 1) + nd * (nc - 1) + 2 * nr * Q * nd + 2 * (nd - 1) * Q


MIB = 2**20


def split_kernel(
    nr, nc, J, QA, QX, go_ref, in_ref, out_ref,
    abuf, at, bbuf, acc, stage, ls, ra, rb, ro, sb, sx, sa, so,
):
    r, c, d = lax.axis_index("row"), lax.axis_index("col"), lax.axis_index("depth")
    e = 1 - d
    core = lax.rem(c, 2)
    sib = c + 1 - 2 * core
    others = [lax.rem(c + 2 * k, nc) for k in range(1, nc // 2)]
    nd = 2
    ta, f = abuf.shape[2], abuf.shape[3]
    w = bbuf.shape[3]
    tb = bbuf.shape[2] // nr
    fh, gh = f // nd, J * w
    ca = ta // QA
    has_up, has_dn = r < nr - 1, r > 0
    up, dn = {"row": jnp.minimum(r + 1, nr - 1)}, {"row": jnp.maximum(r - 1, 0)}
    peer, twin = {"depth": e}, {"col": sib}

    def cols(half, j):
        return pl.ds(pl.multiple_of(half * gh + j * w, 128), w)

    def b_piece(m, b, j):
        return bbuf.at[m, j, pl.ds(pl.multiple_of(b * tb, 128), tb)]

    def a_piece(m, cc, q):
        return abuf.at[m, cc, pl.ds(q * ca, ca)]

    def loop(n, fn, unroll=1):
        lax.fori_loop(0, n, lambda i, _: (fn(i), 0)[1], 0, unroll=unroll)

    def arrived(ref, sem):
        pltpu.make_async_copy(ref, ref, sem).wait()

    def send(src, dst, send_sem, recv_sem, device):
        pltpu.make_async_remote_copy(
            src_ref=src, dst_ref=dst, send_sem=send_sem, recv_sem=recv_sem,
            device_id=device, device_id_type=MESH,
        ).start()

    loop(J, lambda j: pltpu.make_async_copy(in_ref.at[0, :, cols(d, j)], b_piece(d, r, j), ls.at[j]).start())
    load_a = pltpu.make_async_copy(go_ref.at[0], abuf.at[d, c], ls.at[J])
    load_a.start()

    barrier = pltpu.get_barrier_semaphore()

    def greet(device):
        pl.semaphore_signal(barrier, inc=1, device_id=device, device_id_type=MESH)

    pl.when(has_up)(lambda: greet(up))
    pl.when(has_dn)(lambda: greet(dn))
    greet(peer)
    greet(twin)
    for o in others:
        greet({"col": o})
    pl.semaphore_wait(
        barrier, 2 + len(others) + jnp.where(has_up, 1, 0) + jnp.where(has_dn, 1, 0)
    )

    def b_up(m, b, j):
        send(b_piece(m, b, j), b_piece(m, b, j), sb.at[0, m, b, j], rb.at[m, b, j], up)

    def b_dn(m, b, j):
        send(b_piece(m, b, j), b_piece(m, b, j), sb.at[1, m, b, j], rb.at[m, b, j], dn)

    def b_both(m, j):
        pl.when(has_up)(lambda: b_up(m, r, j))
        pl.when(has_dn)(lambda: b_dn(m, r, j))

    def b_wait(m, b, j):
        arrived(b_piece(m, b, j), rb.at[m, b, j])

    def a_send(kind, m, cc, q, device):
        send(a_piece(m, cc, q), a_piece(m, cc, q), sa.at[kind, m, cc, q], ra.at[m, cc, q], device)

    def a_wait(m, cc, q):
        arrived(a_piece(m, cc, q), ra.at[m, cc, q])

    TWIN, PEER, OTHER = 0, 1, 2

    def first(j):
        send(in_ref.at[0, :, cols(e, j)], b_piece(d, r, j), sx.at[j], rb.at[d, r, j], peer)
        pltpu.make_async_copy(in_ref.at[0, :, cols(d, j)], b_piece(d, r, j), ls.at[j]).wait()
        b_both(d, j)

    loop(J, first)
    load_a.wait()

    def own_a(q):
        a_send(PEER, d, c, q, peer)
        for k, o in enumerate(others):
            a_send(OTHER + k, d, c, q, {"col": o})
        a_send(TWIN, d, c, q, twin)

    loop(QA, own_a)

    def second(j):
        b_wait(e, r, j)
        b_both(e, j)

    loop(J, second)

    def pass_on(s, j, wait=True, go=True):
        lo, hi = r - s, r + s
        for m in (d, e):
            @pl.when(jnp.logical_and(lo >= 0, has_up))
            def _():
                if wait:
                    b_wait(m, lo, j)
                if go:
                    b_up(m, lo, j)

            @pl.when(jnp.logical_and(hi < nr, has_dn))
            def _():
                if wait:
                    b_wait(m, hi, j)
                if go:
                    b_dn(m, hi, j)

    LEAD = min(2, J)

    def near(j):
        pl.when(j < J)(lambda: pass_on(1, j, wait=False))

    def far(j):
        @pl.when(j < J)
        def _():
            for s in range(2, nr):
                pass_on(s, j)

    def from_other(q):
        for o in others:
            a_wait(d, o, q)
            a_send(TWIN, d, o, q, twin)
            if q < QX:
                a_send(PEER, d, o, q, peer)

    def from_peer(q):
        a_wait(e, c, q)
        if q >= QX:
            for k, o in enumerate(others):
                a_send(OTHER + k, e, c, q, {"col": o})
        a_send(TWIN, e, c, q, twin)

    def from_corner(q):
        for o in others:
            a_wait(e, o, q)
            a_send(TWIN, e, o, q, twin)

    def from_twin(m):
        for o in [sib] + [lax.rem(sib + 2 * k, nc) for k in range(1, nc // 2)]:
            for q in range(QA):
                a_wait(m, o, q)

    def transpose_a(m):
        def blk(cc):
            def tile(j):
                j0 = pl.multiple_of(j * 128, 128)
                at[m, pl.ds(j0, 128), pl.ds(pl.multiple_of(cc * ta, 128), ta)] = abuf[
                    m, cc, :, pl.ds(j0, 128)
                ].T

            loop(f // 128, tile, unroll=4)

        loop(nc, blk)

    tm = min(512, fh)

    def left(m, b, i):
        return at[m, pl.ds(i * tm, tm), pl.ds(pl.multiple_of(b * tb, 128), tb)]

    def multiply_pair(m, b, p, start=False):
        j = 2 * p
        right = jnp.concatenate([b_piece(m, b, j)[...], b_piece(m, b, j + 1)[...]], axis=1)
        for i in range(f // tm):
            rows = pl.ds(i * tm, tm)
            part = jnp.dot(left(m, b, i), right, preferred_element_type=jnp.float32)
            for k in range(2):
                if start:
                    acc[j + k, rows] = part[:, k * w : (k + 1) * w]
                else:
                    acc[j + k, rows] += part[:, k * w : (k + 1) * w]

    def multiply(m, b, j):
        right = b_piece(m, b, j)[...]
        for i in range(f // tm):
            rows = pl.ds(i * tm, tm)
            acc[j, rows] += jnp.dot(left(m, b, i), right, preferred_element_type=jnp.float32)

    def both_sides(s, fn):
        def side(i):
            b = r + s * (2 * i - 1)
            pl.when(jnp.logical_and(b >= 0, b < nr))(lambda: fn(b))

        loop(2, side)

    def not_passed(b):
        return jnp.logical_or(
            jnp.logical_and(b < r, jnp.logical_not(has_up)),
            jnp.logical_and(b > r, jnp.logical_not(has_dn)),
        )

    def b_here(m, b, j):
        pl.when(not_passed(b))(lambda: b_wait(m, b, j))

    loop(LEAD, lambda j: pass_on(1, j))
    for q in range(QA - 1):
        from_other(q)
    from_peer(0)
    from_other(QA - 1)
    from_peer(1)
    from_twin(d)
    loop(J - LEAD, lambda j: pass_on(1, LEAD + j, go=False))
    transpose_a(d)
    far(0)
    near(LEAD)
    loop(J // 2, lambda p: multiply_pair(d, r, p, start=True))

    def near_block(b):
        loop(J, lambda j: b_here(d, b, j))
        loop(J // 2, lambda p: multiply_pair(d, b, p))

    both_sides(1, near_block)
    from_peer(2)
    from_corner(1)
    far(1)
    near(LEAD + 1)
    for q in range(3, QA):
        from_peer(q)
        from_corner(q - 1)
    far(2)
    near(LEAD + 2)
    from_corner(QA - 1)
    from_corner(0)
    far(3)
    near(LEAD + 3)
    from_twin(e)
    transpose_a(e)

    def column(j):
        def one(s, m, b):
            b_here(m, b, j)
            multiply(m, b, j)

        for s in range(2, nr):
            for m in (d, e):
                both_sides(s, lambda b: one(s, m, b))

        def half(k):
            return acc[j, pl.ds(pl.multiple_of(k * fh, 128), fh)].astype(jnp.bfloat16)

        stage[j] = half(e)
        out_ref[:, cols(d, j)] = half(d)
        send(stage.at[j], out_ref.at[:, cols(d, j)], so.at[j], ro.at[j], peer)

    def pair(p):
        for j in (2 * p, 2 * p + 1):
            far(j + 4)
            near(j + LEAD + 4)
        multiply_pair(e, r, p)

        def near_pair(b):
            for j in (2 * p, 2 * p + 1):
                b_here(e, b, j)
            multiply_pair(e, b, p)

        both_sides(1, near_pair)
        loop(2, lambda k: column(2 * p + k))

    loop(J // 2, pair)

    def drain(j):
        arrived(out_ref.at[:, cols(e, j)], ro.at[j])
        arrived(stage.at[j], so.at[j])
        arrived(b_piece(d, r, j), sx.at[j])
        for m in range(nd):
            def one(b):
                pl.when(jnp.logical_and(has_up, b <= r))(lambda: arrived(b_piece(m, b, j), sb.at[0, m, b, j]))
                pl.when(jnp.logical_and(has_dn, b >= r))(lambda: arrived(b_piece(m, b, j), sb.at[1, m, b, j]))

            loop(nr, one)

    loop(J, drain)

    def drain_a(q):
        def sent(kind, m, cc):
            arrived(a_piece(m, cc, q), sa.at[kind, m, cc, q])

        for m in range(nd):
            for cc in [c] + others:
                sent(TWIN, m, cc)
        sent(PEER, d, c)
        for k in range(len(others)):
            sent(OTHER + k, d, c)
        if q < QX:
            for o in others:
                sent(PEER, d, o)
        else:
            for k in range(len(others)):
                sent(OTHER + k, e, c)

    for q in range(QA):
        drain_a(q)


def split_plan(nr, nc, nd, ta, tb, f, gw):
    w = 128
    if nd != 2 or nc % 2 or nc < 4 or nr < 2 or gw % (nd * 2 * w) or ta % 512 or tb % 128 or f % 1024:
        return None
    J = gw // (nd * w)
    shapes = [
        ((nd, nc, ta, f), jnp.bfloat16),
        ((nd, f, ta * nc), jnp.bfloat16),
        ((nd, J, tb * nr, w), jnp.bfloat16),
        ((J, f, w), jnp.float32),
        ((J, f // nd, w), jnp.bfloat16),
    ]
    size = sum(math.prod(s) * jnp.dtype(t).itemsize for s, t in shapes)
    return (J, shapes) if size <= 52 * MIB else None


def split_body(nr, nc, nd, plan, grad_out, inputs):
    J, shapes = plan
    _, ta, f = grad_out.shape
    gw = inputs.shape[2]
    QA, QX = 4, 1
    return pl.pallas_call(
        functools.partial(split_kernel, nr, nc, J, QA, QX),
        out_shape=pltpu.VMEM((f // nd, gw), jnp.bfloat16),
        in_specs=[pl.BlockSpec(memory_space=pl.ANY)] * 2,
        out_specs=pl.BlockSpec(memory_space=pltpu.VMEM),
        scratch_shapes=[pltpu.VMEM(s, t) for s, t in shapes] + [
            pltpu.SemaphoreType.DMA((J + 1,)),
            pltpu.SemaphoreType.DMA((nd, nc, QA)),
            pltpu.SemaphoreType.DMA((nd, nr, J)),
            pltpu.SemaphoreType.DMA((J,)),
            pltpu.SemaphoreType.DMA((2, nd, nr, J)),
            pltpu.SemaphoreType.DMA((J,)),
            pltpu.SemaphoreType.DMA((1 + nc // 2, nd, nc, QA)),
            pltpu.SemaphoreType.DMA((J,)),
        ],
        compiler_params=pltpu.CompilerParams(
            collective_id=1, has_side_effects=True, vmem_limit_bytes=58 * MIB
        ),
    )(grad_out, inputs)


def body(nr, nc, nd, grad_out, inputs):
    _, ta, f = grad_out.shape
    _, tb, gw = inputs.shape
    fh = f // nd
    Q = max(1, min(4, 32 // (nd * nr)))
    VQ = 3 * Q // 4
    tokens = tb * nr
    plan = split_plan(nr, nc, nd, ta, tb, f, gw)
    if plan is not None:
        return split_body(nr, nc, nd, plan, grad_out, inputs)
    return pl.pallas_call(
        functools.partial(kernel, nr, nc, nd, Q, VQ),
        out_shape=pltpu.VMEM((fh, gw), jnp.bfloat16),
        in_specs=[pl.BlockSpec(memory_space=pl.ANY)] * 2,
        out_specs=pl.BlockSpec(memory_space=pltpu.VMEM),
        scratch_shapes=[
            pltpu.VMEM((nd, nc, ta, fh), jnp.bfloat16),
            pltpu.VMEM((nd, fh, tokens), jnp.bfloat16),
            pltpu.VMEM((nd, nr, tb, gw), jnp.bfloat16),
            pltpu.VMEM((fh, gw), jnp.float32),
            pltpu.SemaphoreType.DMA((2,)),
            pltpu.SemaphoreType.DMA((nd, nc)),
            pltpu.SemaphoreType.DMA((nd, nr, Q)),
            pltpu.SemaphoreType.DMA((count_sends(nr, nc, nd, Q),)),
        ],
        compiler_params=pltpu.CompilerParams(
            collective_id=0, has_side_effects=True, vmem_limit_bytes=52 * 2**20
        ),
    )(grad_out, inputs)


def solution(mesh):
    return jax.shard_map(
        functools.partial(body, mesh.shape["row"], mesh.shape["col"], mesh.shape["depth"]),
        mesh=mesh,
        in_specs=(P("depth", "col", "row"), P("depth", "row", "col")),
        out_specs=P(("row", "depth"), "col"),
        check_vma=False,
    )
```

```python
import functools
import math

import jax
import jax.numpy as jnp
from jax import lax
from jax.experimental import pallas as pl
from jax.experimental.pallas import tpu as pltpu
from jax.sharding import PartitionSpec as P

MESH = pl.DeviceIdType.MESH


def kernel(nr, nc, nd, Q, VQ, go_ref, in_ref, out_ref, abuf, at, bbuf, acc, loc_sem, ra, rb, ss):
    r, c, d = lax.axis_index("row"), lax.axis_index("col"), lax.axis_index("depth")
    ta, fh = abuf.shape[2], abuf.shape[3]
    tb, gw = bbuf.shape[2], bbuf.shape[3]
    cb = tb // Q
    has_up, has_dn = r < nr - 1, r > 0
    pending = []

    load_b = pltpu.make_async_copy(in_ref.at[0], bbuf.at[d, r], loc_sem.at[0])
    load_a = pltpu.make_async_copy(
        go_ref.at[0, :, pl.ds(pl.multiple_of(d * fh, 128), fh)], abuf.at[d, c], loc_sem.at[1]
    )
    load_b.start()
    load_a.start()

    def send(src, dst, recv_sem, device, cond=None):
        copy = pltpu.make_async_remote_copy(
            src_ref=src, dst_ref=dst, send_sem=ss.at[len(pending)], recv_sem=recv_sem,
            device_id=device, device_id_type=MESH,
        )
        pending.append((cond, copy))
        if cond is None:
            copy.start()
        else:
            pl.when(cond)(copy.start)

    def arrived(ref, sem):
        pltpu.make_async_copy(ref, ref, sem).wait()

    def b_chunk(m, b, q):
        return bbuf.at[m, b, pl.ds(q * cb, cb)]

    barrier = pltpu.get_barrier_semaphore()

    @pl.when(has_up)
    def _():
        pl.semaphore_signal(barrier, inc=1, device_id={"row": r + 1}, device_id_type=MESH)

    @pl.when(has_dn)
    def _():
        pl.semaphore_signal(barrier, inc=1, device_id={"row": r - 1}, device_id_type=MESH)

    for k in range(1, nd):
        pl.semaphore_signal(barrier, inc=1, device_id={"depth": lax.rem(d + k, nd)}, device_id_type=MESH)
    for k in range(1, nc):
        pl.semaphore_signal(barrier, inc=1, device_id={"col": lax.rem(c + k, nc)}, device_id_type=MESH)
    neighbours = jnp.where(has_up, 1, 0) + jnp.where(has_dn, 1, 0)
    pl.semaphore_wait(barrier, nd - 1 + nc - 1 + neighbours)

    peers = [lax.rem(d + k, nd) for k in range(1, nd)]

    def to_up(m, b, q, cond):
        send(b_chunk(m, b, q), b_chunk(m, b, q), rb.at[m, b, q], {"row": jnp.minimum(r + 1, nr - 1)}, cond)

    def to_dn(m, b, q, cond):
        send(b_chunk(m, b, q), b_chunk(m, b, q), rb.at[m, b, q], {"row": jnp.maximum(r - 1, 0)}, cond)

    def to_depth(b, q, cond=None):
        for p in peers:
            send(b_chunk(d, b, q), b_chunk(d, b, q), rb.at[d, b, q], {"depth": p}, cond)

    def a_to_col(m):
        for k in range(1, nc):
            send(abuf.at[m, c], abuf.at[m, c], ra.at[m, c], {"col": lax.rem(c + k, nc)})

    for p in peers:
        src = go_ref.at[0, :, pl.ds(pl.multiple_of(p * fh, 128), fh)]
        send(src, abuf.at[d, c], ra.at[d, c], {"depth": p})
    load_b.wait()
    for q in range(Q):
        to_up(d, r, q, has_up)
        to_dn(d, r, q, has_dn)
        to_depth(r, q)
    load_a.wait()
    a_to_col(d)

    def transpose_a(m):
        def blk(cc, _):
            def tile(j, _):
                j0 = pl.multiple_of(j * 128, 128)
                at[m, pl.ds(j0, 128), pl.ds(pl.multiple_of(cc * ta, 128), ta)] = abuf[
                    m, cc, :, pl.ds(j0, 128)
                ].T
                return 0

            return lax.fori_loop(0, fh // 128, tile, 0)

        lax.fori_loop(0, nc, blk, 0)

    tm, tn = min(512, fh), min(512, gw)

    def multiply(m, b, q0, q1, first=False):
        rows = (q1 - q0) * cb

        def tile(i, _):
            i0 = pl.multiple_of((i // (gw // tn)) * tm, tm)
            j0 = pl.multiple_of(lax.rem(i, gw // tn) * tn, tn)
            left = at[m, pl.ds(i0, tm), pl.ds(pl.multiple_of(b * tb + q0 * cb, 128), rows)]
            right = bbuf[m, b, pl.ds(q0 * cb, rows), pl.ds(j0, tn)]
            part = jnp.dot(left, right, preferred_element_type=jnp.float32)
            if first:
                acc[pl.ds(i0, tm), pl.ds(j0, tn)] = part
            else:
                acc[pl.ds(i0, tm), pl.ds(j0, tn)] += part
            return 0

        lax.fori_loop(0, (fh // tm) * (gw // tn), tile, 0)

    def both_sides(s, fn):
        def side(i, _):
            b = r + s * (2 * i - 1)

            @pl.when(jnp.logical_and(b >= 0, b < nr))
            def _():
                fn(b)

            return 0

        lax.fori_loop(0, 2, side, 0)

    def wait_a(m):
        for k in range(1, nc):
            cc = lax.rem(c + k, nc)
            arrived(abuf.at[m, cc], ra.at[m, cc])

    def forward_a():
        for p in peers:
            arrived(abuf.at[p, c], ra.at[p, c])
            a_to_col(p)

    relay_at = max(1, nr - 2)
    for s in range(1, nr):
        lo, hi = r - s, r + s
        for q in range(Q):
            pl.when(lo >= 0)(lambda: arrived(b_chunk(d, lo, q), rb.at[d, lo, q]))
            to_up(d, lo, q, jnp.logical_and(lo >= 0, has_up))
            if not (s == 1 and q < VQ):
                to_depth(lo, q, lo >= 0)
            pl.when(hi < nr)(lambda: arrived(b_chunk(d, hi, q), rb.at[d, hi, q]))
            to_dn(d, hi, q, jnp.logical_and(hi < nr, has_dn))
            if not (s == 1 and q < VQ):
                to_depth(hi, q, hi < nr)
            if s == 1 and q == (Q - 1) // 2:
                forward_a()
        if s == relay_at:
            for p in peers:
                for q in range(Q):
                    arrived(b_chunk(p, r, q), rb.at[p, r, q])
                    if q < VQ:
                        to_up(p, r, q, has_up)
                        to_dn(p, r, q, has_dn)
        if s == 1:
            wait_a(d)
            transpose_a(d)
            multiply(d, r, 0, Q, first=True)
        both_sides(s, lambda b: multiply(d, b, 0, Q))
        if s == relay_at:
            for p in peers:
                wait_a(p)
                transpose_a(p)
                multiply(p, r, 0, Q)

    def take(p, b, q0, q1):
        for q in range(q0, q1):
            arrived(b_chunk(p, b, q), rb.at[p, b, q])
        multiply(p, b, q0, q1)

    half = max(1, Q // 2)
    for s in list(range(2, nr)) + [1]:
        for p in peers:
            for q0 in range(0, Q, half):
                both_sides(s, lambda b: take(p, b, q0, q0 + half))

    def store(i, _):
        i0 = pl.multiple_of(i * 128, 128)
        out_ref[pl.ds(i0, 128), :] = acc[pl.ds(i0, 128), :].astype(out_ref.dtype)
        return 0

    lax.fori_loop(0, fh // 128, store, 0)
    for cond, copy in pending:
        if cond is None:
            copy.wait_send()
        else:
            pl.when(cond)(copy.wait_send)


def count_sends(nr, nc, nd, Q):
    return (nd - 1) + nd * (nc - 1) + 2 * nr * Q * nd + 2 * (nd - 1) * Q


MIB = 2**20


def split_kernel(
    nr, nc, J, QA, QX, go_ref, in_ref, out_ref,
    abuf, at, bbuf, acc, stage, relay, loads, ra, rt, rg, rf, sb, sa, single,
):
    r, c, d = lax.axis_index("row"), lax.axis_index("col"), lax.axis_index("depth")
    e = 1 - d
    core = lax.rem(c, 2)
    sib = c + 1 - 2 * core
    others = [lax.rem(c + 2 * k, nc) for k in range(1, nc // 2)]
    nd = 2
    ta, f = abuf.shape[2], abuf.shape[3]
    w = bbuf.shape[3]
    tb = bbuf.shape[2] // nr
    fh, gh = f // nd, J * w
    ca = ta // QA
    has_up, has_dn = r < nr - 1, r > 0
    up, dn = {"row": jnp.minimum(r + 1, nr - 1)}, {"row": jnp.maximum(r - 1, 0)}
    peer, twin = {"depth": e}, {"col": sib}
    groups = [(0, J // 8), (J // 8, J // 8), (J // 4, J // 4), (J // 2, J // 2)]
    home = c // 2
    sx, so, ro, sr = (single.at[k] for k in range(4))
    tail = jnp.logical_or(r == 1, r == nr - 2)
    tail_row, tail_b = jnp.where(r == 1, 0, nr - 1), jnp.where(r == 1, nr - 1, 0)

    def cols(half, j):
        return pl.ds(pl.multiple_of(half * gh + j * w, 128), w)

    def b_piece(m, b, j):
        return bbuf.at[m, j, tokens(b)]

    def tokens(b):
        return pl.ds(pl.multiple_of(b * tb, 128), tb)

    def a_piece(m, cc, q):
        return abuf.at[m, cc, pl.ds(q * ca, ca)]

    def loop(n, fn, unroll=1):
        lax.fori_loop(0, n, lambda i, _: (fn(i), 0)[1], 0, unroll=unroll)

    def arrived(ref, sem):
        pltpu.make_async_copy(ref, ref, sem).wait()

    def send(src, dst, send_sem, recv_sem, device):
        pltpu.make_async_remote_copy(
            src_ref=src, dst_ref=dst, send_sem=send_sem, recv_sem=recv_sem,
            device_id=device, device_id_type=MESH,
        ).start()

    loop(J, lambda j: pltpu.make_async_copy(in_ref.at[0, :, cols(d, j)], b_piece(d, r, j), loads.at[0]).start())
    load_a = pltpu.make_async_copy(go_ref.at[0], abuf.at[d, c], loads.at[1])
    load_a.start()

    barrier = pltpu.get_barrier_semaphore()

    def greet(device):
        pl.semaphore_signal(barrier, inc=1, device_id=device, device_id_type=MESH)

    pl.when(has_up)(lambda: greet(up))
    pl.when(has_dn)(lambda: greet(dn))
    greet(peer)
    greet(twin)
    for o in others:
        greet({"col": o})
    at_end = jnp.logical_not(jnp.logical_and(has_up, has_dn))

    @pl.when(jnp.logical_and(at_end, core == 0))
    def _():
        greet({"row": jnp.where(r == 0, 1, nr - 2), "col": sib})

    pl.semaphore_wait(
        barrier,
        2 + len(others) + jnp.where(has_up, 1, 0) + jnp.where(has_dn, 1, 0)
        + jnp.where(jnp.logical_and(tail, core == 1), 1, 0),
    )

    def b_send(way, m, b, j, recv_sem):
        send(b_piece(m, b, j), b_piece(m, b, j), sb.at[way, b], recv_sem, (up, dn)[way])

    def b_both(m, g):
        def one(k):
            j = groups[g][0] + k
            pl.when(has_up)(lambda: b_send(0, m, r, j, rg.at[m, r, g]))
            pl.when(has_dn)(lambda: b_send(1, m, r, j, rg.at[m, r, g]))

        loop(groups[g][1], one)

    def group_wait(m, b, g):
        arrived(bbuf.at[m, pl.ds(*groups[g]), tokens(b)], rg.at[m, b, g])

    def far_sem(k, b, j):
        return rf.at[b, j + k * jnp.where(j == J - 1, 1, 0)]

    def far_wait(k, b, j):
        if k == 0:
            pl.when(j < J - 1)(lambda: arrived(bbuf.at[:, j, tokens(b)], rf.at[b, j]))
        pl.when(j == J - 1)(lambda: arrived(b_piece((d, e)[k], b, j), far_sem(k, b, j)))

    def a_send(kind, m, cc, q, device, recv_sem=None):
        recv_sem = ra.at[m, cc // 2, q] if recv_sem is None else recv_sem
        send(a_piece(m, cc, q), a_piece(m, cc, q), sa.at[kind], recv_sem, device)

    def a_twin(m, cc, q, away=0):
        a_send(0, m, cc, q, twin, rt.at[m, away])

    def a_wait(m, cc, q):
        arrived(a_piece(m, cc, q), ra.at[m, cc // 2, q])

    def group_of(j):
        return sum(jnp.where(j >= groups[g][0], 1, 0) for g in range(1, len(groups)))

    loop(J, lambda j: send(in_ref.at[0, :, cols(e, j)], b_piece(d, r, j), sx, rg.at[d, r, group_of(j)], peer))
    arrived(bbuf.at[d, :, tokens(r)], loads.at[0])
    for g in range(len(groups)):
        b_both(d, g)
    load_a.wait()

    def own_a(q):
        a_send(1, d, c, q, peer)
        for k, o in enumerate(others):
            a_send(3 + 2 * k, d, c, q, {"col": o})
        a_twin(d, c, q)

    loop(QA, own_a)
    group_wait(e, r, 0)
    b_both(e, 0)
    for g in range(1, len(groups)):
        group_wait(e, r, g)
        b_both(e, g)

    def pass_near(j):
        for k, m in enumerate((d, e)):
            pl.when(jnp.logical_and(r >= 1, has_up))(lambda: b_send(0, m, r - 1, j, far_sem(k, r - 1, j)))
            pl.when(jnp.logical_and(r + 1 < nr, has_dn))(lambda: b_send(1, m, r + 1, j, far_sem(k, r + 1, j)))

    def wait_near(m, g, passed):
        for b, ok, way in ((r - 1, r >= 1, has_up), (r + 1, r + 1 < nr, has_dn)):
            way = way if passed else jnp.logical_not(way)
            pl.when(jnp.logical_and(ok, way))(lambda: group_wait(m, b, g))

    def pass_far(s, j):
        lo, hi = r - s, r + s
        def go(way, k, b):
            m = (d, e)[k]
            far_wait(k, b, j)
            if s < nr - 2:
                return b_send(way, m, b, j, far_sem(k, b, j))
            aside = jnp.logical_and(j == J - 1, core == 0)
            pl.when(jnp.logical_not(aside))(lambda: b_send(way, m, b, j, far_sem(k, b, j)))
            pl.when(aside)(lambda: send(b_piece(m, b, j), relay.at[k], sr, single.at[4 + k], twin))

        for k in range(2):
            pl.when(jnp.logical_and(lo >= 0, has_up))(lambda: go(0, k, lo))
            pl.when(jnp.logical_and(hi < nr, has_dn))(lambda: go(1, k, hi))

    def pass_relay():
        @pl.when(tail)
        def _():
            for k, m in enumerate((d, e)):
                arrived(relay.at[k], single.at[4 + k])
                send(relay.at[k], b_piece(m, tail_b, J - 1), sr, far_sem(k, tail_b, J - 1), {"row": tail_row, "col": sib})

    LEAD = J // 4

    def near(j):
        pl.when(j < J)(lambda: pass_near(j))

    def far(j):
        @pl.when(j < J)
        def _():
            for s in range(2, nr):
                pass_far(s, j)

    def from_other(q):
        for o in others:
            a_wait(d, o, q)
            a_twin(d, o, q, 1)
            if q < QX:
                a_send(2, d, o, q, peer)

    def from_peer(q):
        a_wait(e, c, q)
        if not isinstance(q, int) or q >= QX:
            for k, o in enumerate(others):
                a_send(4 + 2 * k, e, c, q, {"col": o})
        a_twin(e, c, q)

    def from_corner(q):
        for o in others:
            a_wait(e, o, q)
            a_twin(e, o, q, 1)

    def from_twin(m, away):
        arrived(abuf.at[m, pl.ds(0, len(others) if away else 1)], rt.at[m, away])

    def transpose_a(m, away):
        def blk(i):
            cc = lax.rem(2 * home + 2 * away + i, nc)

            def tile(j):
                j0 = pl.multiple_of(j * 128, 128)
                at[m, pl.ds(j0, 128), pl.ds(pl.multiple_of(cc * ta, 128), ta)] = abuf[
                    m, cc, :, pl.ds(j0, 128)
                ].T

            loop(f // 128, tile, unroll=4)

        loop(nc - 2 if away else 2, blk)

    tm = min(512, fh)

    def left(m, b, i):
        return at[m, pl.ds(i * tm, tm), tokens(b)]

    def multiply_pair(m, b, p):
        j = 2 * p
        right = jnp.concatenate([b_piece(m, b, j)[...], b_piece(m, b, j + 1)[...]], axis=1)
        for i in range(f // tm):
            rows = pl.ds(i * tm, tm)
            part = jnp.dot(left(m, b, i), right, preferred_element_type=jnp.float32)
            for k in range(2):
                acc[j + k, rows] += part[:, k * w : (k + 1) * w]

    def multiply(m, b, j):
        right = b_piece(m, b, j)[...]
        for i in range(f // tm):
            rows = pl.ds(i * tm, tm)
            acc[j, rows] += jnp.dot(left(m, b, i), right, preferred_element_type=jnp.float32)

    def both_sides(s, fn):
        def side(i):
            b = r + s * (2 * i - 1)
            pl.when(jnp.logical_and(b >= 0, b < nr))(lambda: fn(b))

        loop(2, side)

    def not_passed(b):
        return jnp.logical_or(
            jnp.logical_and(b < r, jnp.logical_not(has_up)),
            jnp.logical_and(b > r, jnp.logical_not(has_dn)),
        )

    def at_home(b):
        return b // 2 == home

    def near_blocks(fn, cond=None):
        def one(i):
            b = r - 1 + i
            ok = jnp.logical_and(b >= 0, b < nr)
            pl.when(ok if cond is None else jnp.logical_and(ok, cond(b)))(lambda: fn(b))

        loop(3, one)

    def clear(i):
        acc[i // 4, pl.ds(pl.multiple_of(lax.rem(i, 4) * (f // 4), 128), f // 4)] = jnp.zeros((f // 4, w), jnp.float32)

    loop(4 * J, clear)
    for g in range(2):
        wait_near(d, g, True)
        wait_near(e, g, True)
    loop(LEAD, near)
    from_twin(d, 0)
    transpose_a(d, 0)
    half = QA // 2
    for q in range(half):
        from_other(q)
    for q in range(half):
        from_other(half + q)
        from_peer(q)
    for g in range(2, len(groups)):
        wait_near(d, g, True)
        wait_near(e, g, True)
    for g in range(len(groups)):
        wait_near(d, g, False)
    from_twin(d, 1)
    transpose_a(d, 1)

    def step(t):
        far(t)
        pl.when(t + 1 >= LEAD)(lambda: near(t + 1))

    def first_near(i):
        b = r - 1 + i
        pl.when(jnp.logical_and(b >= 0, b < nr))(lambda: loop(J // 2, lambda p: multiply_pair(d, b, p)))
        from_peer(half + i)
        from_corner(QX + i)
        step(i)

    loop(3, first_near)
    for q in range(half + 3, QA):
        from_peer(q)
        from_corner(q - half + QX)
    step(3)
    from_twin(e, 0)
    for g in range(len(groups)):
        wait_near(e, g, False)
    transpose_a(e, 0)
    near_blocks(lambda b: loop(J // 2, lambda p: multiply_pair(e, b, p)), at_home)

    def far_blocks(fn):
        for s in range(2, nr):
            both_sides(s, fn)

    def early(j):
        def one(b):
            pl.when(not_passed(b))(lambda: far_wait(0, b, j))
            multiply(d, b, j)
            pl.when(at_home(b))(lambda: multiply(e, b, j))

        far_blocks(one)

    for q in range(QA - half + QX, QA - 1):
        from_corner(q)
    for q in range(QX - 1):
        from_corner(q)
    step(4)
    early(0)
    from_corner(QA - 1)
    from_corner(QX - 1)
    early(1)
    from_twin(e, 1)
    transpose_a(e, 1)

    def away(b):
        return jnp.logical_not(at_home(b))

    def finish(j):
        def half_rows(k):
            return acc[j, pl.ds(pl.multiple_of(k * fh, 128), fh)].astype(jnp.bfloat16)

        stage[j] = half_rows(e)
        out_ref[:, cols(d, j)] = half_rows(d)
        send(stage.at[j], out_ref.at[:, cols(d, j)], so, ro, peer)

    def column(j):
        t = j + 4
        pl.when(jnp.logical_and(t > 4, t < J - 1))(lambda: far(t))
        pl.when(jnp.logical_and(t > 4, t < J - 2))(lambda: near(t + 1))

        @pl.when(t == J - 1 + core)
        def _():
            pl.when(core == 1)(pass_relay)
            near(J - 1)
            far(J - 1)

        def one(k, b):
            pl.when(not_passed(b))(lambda: far_wait(k, b, j))
            multiply((d, e)[k], b, j)

        @pl.when(j < 2)
        def _():
            far_blocks(lambda b: pl.when(away(b))(lambda: multiply(e, b, j)))

        @pl.when(j >= 2)
        def _():
            for s in range(2, nr):
                for k in range(2):
                    both_sides(s, lambda b: one(k, b))

        finish(j)

    def pair(p):
        near_blocks(lambda b: multiply_pair(e, b, p), away)
        loop(2, lambda k: column(2 * p + k))

    loop(J // 2, pair)

    arrived(out_ref.at[:, pl.ds(pl.multiple_of(e * gh, 128), gh)], ro)
    arrived(stage, so)
    arrived(bbuf.at[d, :, tokens(r)], sx)

    def drain(b):
        short = jnp.logical_and(jnp.logical_and(tail, core == 0), b == tail_b)
        full = jnp.logical_not(short)
        for way, ok in enumerate((jnp.logical_and(has_up, b <= r), jnp.logical_and(has_dn, b >= r))):
            pl.when(jnp.logical_and(ok, full))(lambda: arrived(bbuf.at[:, :, tokens(b)], sb.at[way, b]))
            pl.when(jnp.logical_and(ok, short))(lambda: arrived(bbuf.at[:, pl.ds(0, J - 1), tokens(b)], sb.at[way, b]))

    loop(nr, drain)
    pl.when(tail)(lambda: arrived(relay, sr))
    arrived(abuf.at[:, pl.ds(0, nc // 2)], sa.at[0])
    arrived(abuf.at[d, c], sa.at[1])
    arrived(abuf.at[d, pl.ds(0, len(others)), pl.ds(0, QX * ca)], sa.at[2])
    for k in range(len(others)):
        arrived(abuf.at[d, c], sa.at[3 + 2 * k])
        arrived(abuf.at[d, c, pl.ds(0, (QA - QX) * ca)], sa.at[4 + 2 * k])


def split_plan(nr, nc, nd, ta, tb, f, gw):
    w = 128
    if nd != 2 or nc % 2 or nc < 4 or nr < 4 or nr != nc or ta != tb or gw % (nd * 8 * w) or ta % 512 or tb % 128 or f % 1024:
        return None
    J = gw // (nd * w)
    shapes = [
        ((nd, nc, ta, f), jnp.bfloat16),
        ((nd, f, ta * nc), jnp.bfloat16),
        ((nd, J, tb * nr, w), jnp.bfloat16),
        ((J, f, w), jnp.float32),
        ((J, f // nd, w), jnp.bfloat16),
        ((2, tb, w), jnp.bfloat16),
    ]
    size = sum(math.prod(s) * jnp.dtype(t).itemsize for s, t in shapes)
    return (J, shapes) if size <= 52 * MIB else None


def split_body(nr, nc, nd, plan, grad_out, inputs):
    J, shapes = plan
    _, ta, f = grad_out.shape
    gw = inputs.shape[2]
    QA, QX = 8, 2
    return pl.pallas_call(
        functools.partial(split_kernel, nr, nc, J, QA, QX),
        out_shape=pltpu.VMEM((f // nd, gw), jnp.bfloat16),
        in_specs=[pl.BlockSpec(memory_space=pl.ANY)] * 2,
        out_specs=pl.BlockSpec(memory_space=pltpu.VMEM),
        scratch_shapes=[pltpu.VMEM(s, t) for s, t in shapes] + [
            pltpu.SemaphoreType.DMA((2,)),
            pltpu.SemaphoreType.DMA((nd, nc // 2, QA)),
            pltpu.SemaphoreType.DMA((nd, 2)),
            pltpu.SemaphoreType.DMA((nd, nr, 4)),
            pltpu.SemaphoreType.DMA((nr, J + 1)),
            pltpu.SemaphoreType.DMA((2, nr)),
            pltpu.SemaphoreType.DMA((1 + nc,)),
            pltpu.SemaphoreType.DMA((6,)),
        ],
        compiler_params=pltpu.CompilerParams(
            collective_id=1, has_side_effects=True, vmem_limit_bytes=58 * MIB
        ),
    )(grad_out, inputs)


def body(nr, nc, nd, grad_out, inputs):
    _, ta, f = grad_out.shape
    _, tb, gw = inputs.shape
    fh = f // nd
    Q = max(1, min(4, 32 // (nd * nr)))
    VQ = 3 * Q // 4
    tokens = tb * nr
    plan = split_plan(nr, nc, nd, ta, tb, f, gw)
    if plan is not None:
        return split_body(nr, nc, nd, plan, grad_out, inputs)
    return pl.pallas_call(
        functools.partial(kernel, nr, nc, nd, Q, VQ),
        out_shape=pltpu.VMEM((fh, gw), jnp.bfloat16),
        in_specs=[pl.BlockSpec(memory_space=pl.ANY)] * 2,
        out_specs=pl.BlockSpec(memory_space=pltpu.VMEM),
        scratch_shapes=[
            pltpu.VMEM((nd, nc, ta, fh), jnp.bfloat16),
            pltpu.VMEM((nd, fh, tokens), jnp.bfloat16),
            pltpu.VMEM((nd, nr, tb, gw), jnp.bfloat16),
            pltpu.VMEM((fh, gw), jnp.float32),
            pltpu.SemaphoreType.DMA((2,)),
            pltpu.SemaphoreType.DMA((nd, nc)),
            pltpu.SemaphoreType.DMA((nd, nr, Q)),
            pltpu.SemaphoreType.DMA((count_sends(nr, nc, nd, Q),)),
        ],
        compiler_params=pltpu.CompilerParams(
            collective_id=0, has_side_effects=True, vmem_limit_bytes=52 * 2**20
        ),
    )(grad_out, inputs)


def solution(mesh):
    return jax.shard_map(
        functools.partial(body, mesh.shape["row"], mesh.shape["col"], mesh.shape["depth"]),
        mesh=mesh,
        in_specs=(P("depth", "col", "row"), P("depth", "row", "col")),
        out_specs=P(("row", "depth"), "col"),
        check_vma=False,
    )
```

```python
import functools
import math

import jax
import jax.numpy as jnp
from jax import lax
from jax.experimental import pallas as pl
from jax.experimental.pallas import tpu as pltpu
from jax.sharding import PartitionSpec as P

MESH = pl.DeviceIdType.MESH


def kernel(nr, nc, nd, Q, VQ, go_ref, in_ref, out_ref, abuf, at, bbuf, acc, loc_sem, ra, rb, ss):
    r, c, d = lax.axis_index("row"), lax.axis_index("col"), lax.axis_index("depth")
    ta, fh = abuf.shape[2], abuf.shape[3]
    tb, gw = bbuf.shape[2], bbuf.shape[3]
    cb = tb // Q
    has_up, has_dn = r < nr - 1, r > 0
    pending = []

    load_b = pltpu.make_async_copy(in_ref.at[0], bbuf.at[d, r], loc_sem.at[0])
    load_a = pltpu.make_async_copy(
        go_ref.at[0, :, pl.ds(pl.multiple_of(d * fh, 128), fh)], abuf.at[d, c], loc_sem.at[1]
    )
    load_b.start()
    load_a.start()

    def send(src, dst, recv_sem, device, cond=None):
        copy = pltpu.make_async_remote_copy(
            src_ref=src, dst_ref=dst, send_sem=ss.at[len(pending)], recv_sem=recv_sem,
            device_id=device, device_id_type=MESH,
        )
        pending.append((cond, copy))
        if cond is None:
            copy.start()
        else:
            pl.when(cond)(copy.start)

    def arrived(ref, sem):
        pltpu.make_async_copy(ref, ref, sem).wait()

    def b_chunk(m, b, q):
        return bbuf.at[m, b, pl.ds(q * cb, cb)]

    barrier = pltpu.get_barrier_semaphore()

    @pl.when(has_up)
    def _():
        pl.semaphore_signal(barrier, inc=1, device_id={"row": r + 1}, device_id_type=MESH)

    @pl.when(has_dn)
    def _():
        pl.semaphore_signal(barrier, inc=1, device_id={"row": r - 1}, device_id_type=MESH)

    for k in range(1, nd):
        pl.semaphore_signal(barrier, inc=1, device_id={"depth": lax.rem(d + k, nd)}, device_id_type=MESH)
    for k in range(1, nc):
        pl.semaphore_signal(barrier, inc=1, device_id={"col": lax.rem(c + k, nc)}, device_id_type=MESH)
    neighbours = jnp.where(has_up, 1, 0) + jnp.where(has_dn, 1, 0)
    pl.semaphore_wait(barrier, nd - 1 + nc - 1 + neighbours)

    peers = [lax.rem(d + k, nd) for k in range(1, nd)]

    def to_up(m, b, q, cond):
        send(b_chunk(m, b, q), b_chunk(m, b, q), rb.at[m, b, q], {"row": jnp.minimum(r + 1, nr - 1)}, cond)

    def to_dn(m, b, q, cond):
        send(b_chunk(m, b, q), b_chunk(m, b, q), rb.at[m, b, q], {"row": jnp.maximum(r - 1, 0)}, cond)

    def to_depth(b, q, cond=None):
        for p in peers:
            send(b_chunk(d, b, q), b_chunk(d, b, q), rb.at[d, b, q], {"depth": p}, cond)

    def a_to_col(m):
        for k in range(1, nc):
            send(abuf.at[m, c], abuf.at[m, c], ra.at[m, c], {"col": lax.rem(c + k, nc)})

    for p in peers:
        src = go_ref.at[0, :, pl.ds(pl.multiple_of(p * fh, 128), fh)]
        send(src, abuf.at[d, c], ra.at[d, c], {"depth": p})
    load_b.wait()
    for q in range(Q):
        to_up(d, r, q, has_up)
        to_dn(d, r, q, has_dn)
        to_depth(r, q)
    load_a.wait()
    a_to_col(d)

    def transpose_a(m):
        def blk(cc, _):
            def tile(j, _):
                j0 = pl.multiple_of(j * 128, 128)
                at[m, pl.ds(j0, 128), pl.ds(pl.multiple_of(cc * ta, 128), ta)] = abuf[
                    m, cc, :, pl.ds(j0, 128)
                ].T
                return 0

            return lax.fori_loop(0, fh // 128, tile, 0)

        lax.fori_loop(0, nc, blk, 0)

    tm, tn = min(512, fh), min(512, gw)

    def multiply(m, b, q0, q1, first=False):
        rows = (q1 - q0) * cb

        def tile(i, _):
            i0 = pl.multiple_of((i // (gw // tn)) * tm, tm)
            j0 = pl.multiple_of(lax.rem(i, gw // tn) * tn, tn)
            left = at[m, pl.ds(i0, tm), pl.ds(pl.multiple_of(b * tb + q0 * cb, 128), rows)]
            right = bbuf[m, b, pl.ds(q0 * cb, rows), pl.ds(j0, tn)]
            part = jnp.dot(left, right, preferred_element_type=jnp.float32)
            if first:
                acc[pl.ds(i0, tm), pl.ds(j0, tn)] = part
            else:
                acc[pl.ds(i0, tm), pl.ds(j0, tn)] += part
            return 0

        lax.fori_loop(0, (fh // tm) * (gw // tn), tile, 0)

    def both_sides(s, fn):
        def side(i, _):
            b = r + s * (2 * i - 1)

            @pl.when(jnp.logical_and(b >= 0, b < nr))
            def _():
                fn(b)

            return 0

        lax.fori_loop(0, 2, side, 0)

    def wait_a(m):
        for k in range(1, nc):
            cc = lax.rem(c + k, nc)
            arrived(abuf.at[m, cc], ra.at[m, cc])

    def forward_a():
        for p in peers:
            arrived(abuf.at[p, c], ra.at[p, c])
            a_to_col(p)

    relay_at = max(1, nr - 2)
    for s in range(1, nr):
        lo, hi = r - s, r + s
        for q in range(Q):
            pl.when(lo >= 0)(lambda: arrived(b_chunk(d, lo, q), rb.at[d, lo, q]))
            to_up(d, lo, q, jnp.logical_and(lo >= 0, has_up))
            if not (s == 1 and q < VQ):
                to_depth(lo, q, lo >= 0)
            pl.when(hi < nr)(lambda: arrived(b_chunk(d, hi, q), rb.at[d, hi, q]))
            to_dn(d, hi, q, jnp.logical_and(hi < nr, has_dn))
            if not (s == 1 and q < VQ):
                to_depth(hi, q, hi < nr)
            if s == 1 and q == (Q - 1) // 2:
                forward_a()
        if s == relay_at:
            for p in peers:
                for q in range(Q):
                    arrived(b_chunk(p, r, q), rb.at[p, r, q])
                    if q < VQ:
                        to_up(p, r, q, has_up)
                        to_dn(p, r, q, has_dn)
        if s == 1:
            wait_a(d)
            transpose_a(d)
            multiply(d, r, 0, Q, first=True)
        both_sides(s, lambda b: multiply(d, b, 0, Q))
        if s == relay_at:
            for p in peers:
                wait_a(p)
                transpose_a(p)
                multiply(p, r, 0, Q)

    def take(p, b, q0, q1):
        for q in range(q0, q1):
            arrived(b_chunk(p, b, q), rb.at[p, b, q])
        multiply(p, b, q0, q1)

    half = max(1, Q // 2)
    for s in list(range(2, nr)) + [1]:
        for p in peers:
            for q0 in range(0, Q, half):
                both_sides(s, lambda b: take(p, b, q0, q0 + half))

    def store(i, _):
        i0 = pl.multiple_of(i * 128, 128)
        out_ref[pl.ds(i0, 128), :] = acc[pl.ds(i0, 128), :].astype(out_ref.dtype)
        return 0

    lax.fori_loop(0, fh // 128, store, 0)
    for cond, copy in pending:
        if cond is None:
            copy.wait_send()
        else:
            pl.when(cond)(copy.wait_send)


def count_sends(nr, nc, nd, Q):
    return (nd - 1) + nd * (nc - 1) + 2 * nr * Q * nd + 2 * (nd - 1) * Q


MIB = 2**20


def split_kernel(
    nr, nc, J, QA, QX, go_ref, in_ref, out_ref,
    abuf, at, bbuf, acc, stage, relay, loads, ro2, rp, rc, rt, rx, rn, rf, sb, sa, single,
):
    r, c, d = lax.axis_index("row"), lax.axis_index("col"), lax.axis_index("depth")
    e = 1 - d
    core = lax.rem(c, 2)
    sib = c + 1 - 2 * core
    others = [lax.rem(c + 2 * k, nc) for k in range(1, nc // 2)]
    nd = 2
    ta, f = abuf.shape[2], abuf.shape[3]
    w = bbuf.shape[3]
    tb = bbuf.shape[2] // nr
    fh, gh = f // nd, J * w
    ca = ta // QA
    has_up, has_dn = r < nr - 1, r > 0
    up, dn = {"row": jnp.minimum(r + 1, nr - 1)}, {"row": jnp.maximum(r - 1, 0)}
    peer, twin = {"depth": e}, {"col": sib}
    groups = [(0, J // 4), (J // 4, J // 4), (J // 2, J // 2)]
    home = c // 2
    LEAD = J // 4
    sx, so, ro, sr = (single.at[k] for k in range(4))
    tail = jnp.logical_or(r == 1, r == nr - 2)
    tail_row, tail_b = jnp.where(r == 1, 0, nr - 1), jnp.where(r == 1, nr - 1, 0)

    def cols(half, j):
        return pl.ds(pl.multiple_of(half * gh + j * w, 128), w)

    def b_piece(m, b, j):
        return bbuf.at[m, j, tokens(b)]

    def tokens(b):
        return pl.ds(pl.multiple_of(b * tb, 128), tb)

    def a_piece(m, cc, q):
        return abuf.at[m, cc, pl.ds(q * ca, ca)]

    def loop(n, fn, unroll=1):
        lax.fori_loop(0, n, lambda i, _: (fn(i), 0)[1], 0, unroll=unroll)

    def arrived(ref, sem):
        pltpu.make_async_copy(ref, ref, sem).wait()

    def send(src, dst, send_sem, recv_sem, device):
        pltpu.make_async_remote_copy(
            src_ref=src, dst_ref=dst, send_sem=send_sem, recv_sem=recv_sem,
            device_id=device, device_id_type=MESH,
        ).start()

    loop(J, lambda j: pltpu.make_async_copy(in_ref.at[0, :, cols(d, j)], b_piece(d, r, j), loads.at[0]).start())
    load_a = pltpu.make_async_copy(go_ref.at[0], abuf.at[d, c], loads.at[1])
    load_a.start()

    barrier = pltpu.get_barrier_semaphore()

    def greet(device):
        pl.semaphore_signal(barrier, inc=1, device_id=device, device_id_type=MESH)

    pl.when(has_up)(lambda: greet(up))
    pl.when(has_dn)(lambda: greet(dn))
    greet(peer)
    greet(twin)
    for o in others:
        greet({"col": o})
    at_end = jnp.logical_not(jnp.logical_and(has_up, has_dn))

    @pl.when(jnp.logical_and(at_end, core == 0))
    def _():
        greet({"row": jnp.where(r == 0, 1, nr - 2), "col": sib})

    pl.semaphore_wait(
        barrier,
        2 + len(others) + jnp.where(has_up, 1, 0) + jnp.where(has_dn, 1, 0)
        + jnp.where(jnp.logical_and(tail, core == 1), 1, 0),
    )

    def b_send(way, m, b, j, recv_sem):
        send(b_piece(m, b, j), b_piece(m, b, j), sb.at[way, b], recv_sem, (up, dn)[way])

    def b_both(k, g):
        m = (d, e)[k]

        def one(i):
            j = groups[g][0] + i
            pl.when(has_up)(lambda: b_send(0, m, r, j, rn.at[0, k, min(g, 1)]))
            pl.when(has_dn)(lambda: b_send(1, m, r, j, rn.at[1, k, min(g, 1)]))

        loop(groups[g][1], one)

    def group_wait(g):
        arrived(bbuf.at[e, pl.ds(*groups[g]), tokens(r)], rx.at[g])

    def near_wait(k, b, side, g):
        span = pl.ds(0, LEAD) if g == 0 else pl.ds(LEAD, J - LEAD)
        arrived(bbuf.at[(d, e)[k], span, tokens(b)], rn.at[side, k, g])

    def far_slot(b, row):
        return jnp.where(b < row, b, b - 2 - jnp.where(row > 0, 1, 0))

    def far_sem(k, b, j, row):
        return rf.at[far_slot(b, row), j + k * jnp.where(j == J - 1, 1, 0)]

    def far_wait(k, b, j):
        m = jnp.where(k == 0, d, e)
        pl.when(jnp.logical_and(k == 0, j < J - 1))(lambda: arrived(bbuf.at[:, j, tokens(b)], rf.at[far_slot(b, r), j]))
        pl.when(j == J - 1)(lambda: arrived(b_piece(m, b, j), far_sem(k, b, j, r)))

    def corner_sem(o, q):
        return rc.at[o // 2, q // 2 + jnp.where(q == QA - 1, 1, 0)]

    def a_send(kind, m, cc, q, device, recv_sem):
        send(a_piece(m, cc, q), a_piece(m, cc, q), sa.at[kind], recv_sem, device)

    def a_twin(m, cc, q, away=0):
        a_send(0, m, cc, q, twin, rt.at[m, away])

    def group_of(j):
        return sum(jnp.where(j >= groups[g][0], 1, 0) for g in range(1, len(groups)))

    arrived(bbuf.at[d, :, tokens(r)], loads.at[0])
    b_both(0, 0)
    loop(J, lambda j: send(in_ref.at[0, :, cols(e, j)], b_piece(d, r, j), sx, rx.at[group_of(j)], peer))
    for g in range(1, len(groups)):
        b_both(0, g)
    load_a.wait()

    def own_a(q):
        a_send(1, d, c, q, peer, rp.at[q])
        for k, o in enumerate(others):
            a_send(3 + 2 * k, d, c, q, {"col": o}, ro2.at[home, q // 2])
        a_twin(d, c, q)

    loop(QA, own_a)
    group_wait(0)
    b_both(1, 0)
    for g in range(1, len(groups)):
        group_wait(g)
        b_both(1, g)

    def pass_near(j):
        for k, m in enumerate((d, e)):
            pl.when(jnp.logical_and(r >= 1, has_up))(lambda: b_send(0, m, r - 1, j, far_sem(k, r - 1, j, r + 1)))
            pl.when(jnp.logical_and(r + 1 < nr, has_dn))(lambda: b_send(1, m, r + 1, j, far_sem(k, r + 1, j, r - 1)))

    def wait_near(k, g, passed):
        for side, b, ok, way in ((0, r - 1, r >= 1, has_up), (1, r + 1, r + 1 < nr, has_dn)):
            way = way if passed else jnp.logical_not(way)
            pl.when(jnp.logical_and(ok, way))(lambda: near_wait(k, b, side, g))

    def pass_far(s, j):
        lo, hi = r - s, r + s
        def go(way, k, b):
            m = (d, e)[k]
            far_wait(k, b, j)
            if s < nr - 2:
                return b_send(way, m, b, j, far_sem(k, b, j, (r + 1, r - 1)[way]))
            aside = jnp.logical_and(j == J - 1, core == 0)
            pl.when(jnp.logical_not(aside))(lambda: b_send(way, m, b, j, far_sem(k, b, j, (r + 1, r - 1)[way])))
            pl.when(aside)(lambda: send(b_piece(m, b, j), relay.at[k], sr, single.at[4 + k], twin))

        for k in range(2):
            pl.when(jnp.logical_and(lo >= 0, has_up))(lambda: go(0, k, lo))
            pl.when(jnp.logical_and(hi < nr, has_dn))(lambda: go(1, k, hi))

    def pass_relay():
        @pl.when(tail)
        def _():
            for k, m in enumerate((d, e)):
                arrived(relay.at[k], single.at[4 + k])
                send(relay.at[k], b_piece(m, tail_b, J - 1), sr, far_sem(k, tail_b, J - 1, tail_row), {"row": tail_row, "col": sib})

    def near(j):
        pl.when(j < J)(lambda: pass_near(j))

    def far(j):
        @pl.when(j < J)
        def _():
            for s in range(2, nr):
                pass_far(s, j)

    def pair_wait(m, cc, q, sem):
        arrived(abuf.at[m, cc, pl.ds(q * ca, 2 * ca)], sem)

    def from_other(q):
        for o in others:
            if q % 2 == 0:
                pair_wait(d, o, q, ro2.at[o // 2, q // 2])
            a_twin(d, o, q, 1)
            if q < QX:
                a_send(2, d, o, q, peer, corner_sem(o, q))

    def from_peer(q):
        arrived(a_piece(e, c, q), rp.at[q])
        if not isinstance(q, int) or q >= QX:
            for k, o in enumerate(others):
                a_send(4 + 2 * k, e, c, q, {"col": o}, corner_sem(c, q))
        a_twin(e, c, q)

    def from_corner(q):
        for o in others:
            @pl.when(q >= QA - 2)
            def _():
                arrived(a_piece(e, o, q), corner_sem(o, q))
                a_twin(e, o, q, 1)

            @pl.when(jnp.logical_and(q < QA - 2, lax.rem(q, 2) == 1))
            def _():
                pair_wait(e, o, q - 1, corner_sem(o, q))
                a_twin(e, o, q - 1, 1)
                a_twin(e, o, q, 1)

    def from_twin(m, away):
        arrived(abuf.at[m, pl.ds(0, len(others) if away else 1)], rt.at[m, away])

    def transpose_a(m, away):
        def blk(i):
            cc = lax.rem(2 * home + 2 * away + i, nc)

            def tile(j):
                j0 = pl.multiple_of(j * 128, 128)
                at[m, pl.ds(j0, 128), pl.ds(pl.multiple_of(cc * ta, 128), ta)] = abuf[
                    m, cc, :, pl.ds(j0, 128)
                ].T

            loop(f // 128, tile, unroll=4)

        loop(nc - 2 if away else 2, blk)

    tm = min(512, fh)

    def left(m, b, i):
        return at[m, pl.ds(i * tm, tm), tokens(b)]

    def multiply_pair(m, b, p):
        j = 2 * p
        right = jnp.concatenate([b_piece(m, b, j)[...], b_piece(m, b, j + 1)[...]], axis=1)
        for i in range(f // tm):
            rows = pl.ds(i * tm, tm)
            part = jnp.dot(left(m, b, i), right, preferred_element_type=jnp.float32)
            for k in range(2):
                acc[j + k, rows] += part[:, k * w : (k + 1) * w]

    def multiply(m, b, j):
        right = b_piece(m, b, j)[...]
        for i in range(f // tm):
            rows = pl.ds(i * tm, tm)
            acc[j, rows] += jnp.dot(left(m, b, i), right, preferred_element_type=jnp.float32)

    def not_passed(b):
        return jnp.logical_or(
            jnp.logical_and(b < r, jnp.logical_not(has_up)),
            jnp.logical_and(b > r, jnp.logical_not(has_dn)),
        )

    def at_home(b):
        return b // 2 == home

    def near_blocks(fn, cond=None):
        def one(i):
            b = r - 1 + i
            ok = jnp.logical_and(b >= 0, b < nr)
            pl.when(ok if cond is None else jnp.logical_and(ok, cond(b)))(lambda: fn(b))

        loop(3, one)

    def clear(i):
        acc[i // 4, pl.ds(pl.multiple_of(lax.rem(i, 4) * (f // 4), 128), f // 4)] = jnp.zeros((f // 4, w), jnp.float32)

    loop(4 * J, clear)
    wait_near(0, 0, True)
    wait_near(1, 0, True)
    loop(LEAD, near)
    from_twin(d, 0)
    transpose_a(d, 0)
    half = QA // 2
    for q in range(half):
        from_other(q)
    for q in range(half):
        from_other(half + q)
        from_peer(q)
    wait_near(0, 1, True)
    wait_near(1, 1, True)
    for g in range(2):
        wait_near(0, g, False)
    from_twin(d, 1)
    transpose_a(d, 1)

    def step(t):
        far(t)
        pl.when(t + 1 >= LEAD)(lambda: near(t + 1))

    def first_near(i):
        b = r - 1 + i
        pl.when(jnp.logical_and(b >= 0, b < nr))(lambda: loop(J // 2, lambda p: multiply_pair(d, b, p)))
        from_peer(half + i)
        from_corner(QX + i)
        step(i)

    loop(3, first_near)
    for q in range(half + 3, QA):
        from_peer(q)
        from_corner(q - half + QX)
    step(3)
    from_twin(e, 0)
    for g in range(2):
        wait_near(1, g, False)
    transpose_a(e, 0)
    near_blocks(lambda b: loop(J // 2, lambda p: multiply_pair(e, b, p)), at_home)

    def far_blocks(fn):
        def one(i):
            s, b = 2 + i // 2, r + (2 + i // 2) * (2 * lax.rem(i, 2) - 1)
            pl.when(jnp.logical_and(b >= 0, b < nr))(lambda: fn(s, b))

        loop(2 * (nr - 2), one)

    def early(j):
        def one(s, b):
            pl.when(not_passed(b))(lambda: far_wait(0, b, j))

            def part(k):
                pl.when(jnp.logical_or(k == 0, at_home(b)))(lambda: multiply(jnp.where(k == 0, d, e), b, j))

            loop(2, part)

        far_blocks(one)

    for q in range(QA - half + QX, QA - 1):
        from_corner(q)
    for q in range(QX - 1):
        from_corner(q)
    step(4)
    early(0)
    from_corner(QA - 1)
    from_corner(QX - 1)
    early(1)
    from_twin(e, 1)
    transpose_a(e, 1)

    def away(b):
        return jnp.logical_not(at_home(b))

    span = jnp.logical_or(r == 0, r == nr - 1)
    end_b = jnp.where(r == 0, nr - 1, 0)
    hh = fh // 4

    def settle_sends():
        arrived(bbuf.at[d, :, tokens(r)], sx)
        arrived(abuf.at[:, pl.ds(0, nc // 2)], sa.at[0])
        arrived(abuf.at[d, c], sa.at[1])
        arrived(abuf.at[d, pl.ds(0, len(others)), pl.ds(0, QX * ca)], sa.at[2])
        for k in range(len(others)):
            arrived(abuf.at[d, c], sa.at[3 + 2 * k])
            arrived(abuf.at[d, c, pl.ds(0, (QA - QX) * ca)], sa.at[4 + 2 * k])
        pl.when(has_up)(lambda: arrived(bbuf.at[:, :, tokens(r)], sb.at[0, r]))
        pl.when(has_dn)(lambda: arrived(bbuf.at[:, :, tokens(r)], sb.at[1, r]))

    def column(j):
        t = j + 4
        pl.when(jnp.logical_and(t > 4, t < J - 1))(lambda: far(t))
        pl.when(jnp.logical_and(t > 4, t < J - 2))(lambda: near(t + 1))

        @pl.when(t == J - 1 + core)
        def _():
            pl.when(core == 1)(pass_relay)
            near(J - 1)
            far(J - 1)

        def block(s, b):
            def part(k):
                todo = jnp.logical_or(j >= 2, jnp.logical_and(k == 1, away(b)))
                todo = jnp.logical_and(todo, jnp.logical_or(s < nr - 1, k == 0))

                @pl.when(todo)
                def _():
                    pl.when(jnp.logical_and(j >= 2, not_passed(b)))(lambda: far_wait(k, b, j))
                    multiply(jnp.where(k == 0, d, e), b, j)

            loop(2, part)

        far_blocks(block)
        pl.when(j == J - 1)(settle_sends)
        left_over = jnp.logical_and(span, jnp.logical_or(j >= 2, away(end_b)))
        pl.when(jnp.logical_and(left_over, j >= 2))(lambda: far_wait(1, end_b, j))

        def leave(i):
            rows = pl.ds(pl.multiple_of(i * hh, 128), hh)
            send(stage.at[j, rows], out_ref.at[rows, cols(d, j)], so, ro, peer)

        def quarter(i):
            rows = pl.ds(pl.multiple_of(jnp.where(i < 4, e, d) * fh + lax.rem(i, 4) * hh, 128), hh)

            @pl.when(left_over)
            def _():
                acc[j, rows] += jnp.dot(
                    at[e, rows, tokens(end_b)], b_piece(e, end_b, j)[...], preferred_element_type=jnp.float32
                )

            here = pl.ds(pl.multiple_of(lax.rem(i, 4) * hh, 128), hh)
            done = acc[j, rows].astype(jnp.bfloat16)

            @pl.when(i < 4)
            def _():
                stage[j, here] = done

            @pl.when(i >= 4)
            def _():
                out_ref[here, cols(d, j)] = done

            pl.when(jnp.logical_and(i >= 1, i < 5))(lambda: leave(i - 1))

        loop(8, quarter)

    def pair(p):
        near_blocks(lambda b: multiply_pair(e, b, p), away)
        loop(2, lambda k: column(2 * p + k))

    loop(J // 2, pair)

    def drain(b):
        short = jnp.logical_and(jnp.logical_and(tail, core == 0), b == tail_b)
        full = jnp.logical_not(jnp.logical_or(short, b == r))
        for way, ok in enumerate((jnp.logical_and(has_up, b <= r), jnp.logical_and(has_dn, b >= r))):
            pl.when(jnp.logical_and(ok, full))(lambda: arrived(bbuf.at[:, :, tokens(b)], sb.at[way, b]))
            pl.when(jnp.logical_and(ok, short))(lambda: arrived(bbuf.at[:, pl.ds(0, J - 1), tokens(b)], sb.at[way, b]))

    loop(nr, drain)
    pl.when(tail)(lambda: arrived(relay, sr))
    arrived(stage, so)
    arrived(out_ref.at[:, pl.ds(pl.multiple_of(e * gh, 128), gh)], ro)


def split_plan(nr, nc, nd, ta, tb, f, gw):
    w = 128
    if nd != 2 or nc % 2 or nc < 4 or nr < 4 or nr != nc or ta != tb or gw % (nd * 8 * w) or ta % 512 or tb % 128 or f % 1024:
        return None
    J = gw // (nd * w)
    shapes = [
        ((nd, nc, ta, f), jnp.bfloat16),
        ((nd, f, ta * nc), jnp.bfloat16),
        ((nd, J, tb * nr, w), jnp.bfloat16),
        ((J, f, w), jnp.float32),
        ((J, f // nd, w), jnp.bfloat16),
        ((2, tb, w), jnp.bfloat16),
    ]
    size = sum(math.prod(s) * jnp.dtype(t).itemsize for s, t in shapes)
    return (J, shapes) if size <= 52 * MIB else None


def split_body(nr, nc, nd, plan, grad_out, inputs):
    J, shapes = plan
    _, ta, f = grad_out.shape
    gw = inputs.shape[2]
    QA, QX = 8, 2
    return pl.pallas_call(
        functools.partial(split_kernel, nr, nc, J, QA, QX),
        out_shape=pltpu.VMEM((f // nd, gw), jnp.bfloat16),
        in_specs=[pl.BlockSpec(memory_space=pl.ANY)] * 2,
        out_specs=pl.BlockSpec(memory_space=pltpu.VMEM),
        scratch_shapes=[pltpu.VMEM(s, t) for s, t in shapes] + [
            pltpu.SemaphoreType.DMA((2,)),
            pltpu.SemaphoreType.DMA((nc // 2, QA // 2)),
            pltpu.SemaphoreType.DMA((QA,)),
            pltpu.SemaphoreType.DMA((nc // 2, QA // 2 + 1)),
            pltpu.SemaphoreType.DMA((nd, 2)),
            pltpu.SemaphoreType.DMA((3,)),
            pltpu.SemaphoreType.DMA((2, 2, 2)),
            pltpu.SemaphoreType.DMA((nr - 2, J + 1)),
            pltpu.SemaphoreType.DMA((2, nr)),
            pltpu.SemaphoreType.DMA((1 + nc,)),
            pltpu.SemaphoreType.DMA((6,)),
        ],
        compiler_params=pltpu.CompilerParams(
            collective_id=1, has_side_effects=True, vmem_limit_bytes=58 * MIB
        ),
    )(grad_out, inputs)


def body(nr, nc, nd, grad_out, inputs):
    _, ta, f = grad_out.shape
    _, tb, gw = inputs.shape
    fh = f // nd
    Q = max(1, min(4, 32 // (nd * nr)))
    VQ = 3 * Q // 4
    tokens = tb * nr
    plan = split_plan(nr, nc, nd, ta, tb, f, gw)
    if plan is not None:
        return split_body(nr, nc, nd, plan, grad_out, inputs)
    return pl.pallas_call(
        functools.partial(kernel, nr, nc, nd, Q, VQ),
        out_shape=pltpu.VMEM((fh, gw), jnp.bfloat16),
        in_specs=[pl.BlockSpec(memory_space=pl.ANY)] * 2,
        out_specs=pl.BlockSpec(memory_space=pltpu.VMEM),
        scratch_shapes=[
            pltpu.VMEM((nd, nc, ta, fh), jnp.bfloat16),
            pltpu.VMEM((nd, fh, tokens), jnp.bfloat16),
            pltpu.VMEM((nd, nr, tb, gw), jnp.bfloat16),
            pltpu.VMEM((fh, gw), jnp.float32),
            pltpu.SemaphoreType.DMA((2,)),
            pltpu.SemaphoreType.DMA((nd, nc)),
            pltpu.SemaphoreType.DMA((nd, nr, Q)),
            pltpu.SemaphoreType.DMA((count_sends(nr, nc, nd, Q),)),
        ],
        compiler_params=pltpu.CompilerParams(
            collective_id=0, has_side_effects=True, vmem_limit_bytes=52 * 2**20
        ),
    )(grad_out, inputs)


def solution(mesh):
    return jax.shard_map(
        functools.partial(body, mesh.shape["row"], mesh.shape["col"], mesh.shape["depth"]),
        mesh=mesh,
        in_specs=(P("depth", "col", "row"), P("depth", "row", "col")),
        out_specs=P(("row", "depth"), "col"),
        check_vma=False,
    )
```

```python
import functools
import math

import jax
import jax.numpy as jnp
from jax import lax
from jax.experimental import pallas as pl
from jax.experimental.pallas import tpu as pltpu
from jax.sharding import PartitionSpec as P

MESH = pl.DeviceIdType.MESH


def kernel(nr, nc, nd, Q, VQ, go_ref, in_ref, out_ref, abuf, at, bbuf, acc, loc_sem, ra, rb, ss):
    r, c, d = lax.axis_index("row"), lax.axis_index("col"), lax.axis_index("depth")
    ta, fh = abuf.shape[2], abuf.shape[3]
    tb, gw = bbuf.shape[2], bbuf.shape[3]
    cb = tb // Q
    has_up, has_dn = r < nr - 1, r > 0
    pending = []

    load_b = pltpu.make_async_copy(in_ref.at[0], bbuf.at[d, r], loc_sem.at[0])
    load_a = pltpu.make_async_copy(
        go_ref.at[0, :, pl.ds(pl.multiple_of(d * fh, 128), fh)], abuf.at[d, c], loc_sem.at[1]
    )
    load_b.start()
    load_a.start()

    def send(src, dst, recv_sem, device, cond=None):
        copy = pltpu.make_async_remote_copy(
            src_ref=src, dst_ref=dst, send_sem=ss.at[len(pending)], recv_sem=recv_sem,
            device_id=device, device_id_type=MESH,
        )
        pending.append((cond, copy))
        if cond is None:
            copy.start()
        else:
            pl.when(cond)(copy.start)

    def arrived(ref, sem):
        pltpu.make_async_copy(ref, ref, sem).wait()

    def b_chunk(m, b, q):
        return bbuf.at[m, b, pl.ds(q * cb, cb)]

    barrier = pltpu.get_barrier_semaphore()

    @pl.when(has_up)
    def _():
        pl.semaphore_signal(barrier, inc=1, device_id={"row": r + 1}, device_id_type=MESH)

    @pl.when(has_dn)
    def _():
        pl.semaphore_signal(barrier, inc=1, device_id={"row": r - 1}, device_id_type=MESH)

    for k in range(1, nd):
        pl.semaphore_signal(barrier, inc=1, device_id={"depth": lax.rem(d + k, nd)}, device_id_type=MESH)
    for k in range(1, nc):
        pl.semaphore_signal(barrier, inc=1, device_id={"col": lax.rem(c + k, nc)}, device_id_type=MESH)
    neighbours = jnp.where(has_up, 1, 0) + jnp.where(has_dn, 1, 0)
    pl.semaphore_wait(barrier, nd - 1 + nc - 1 + neighbours)

    peers = [lax.rem(d + k, nd) for k in range(1, nd)]

    def to_up(m, b, q, cond):
        send(b_chunk(m, b, q), b_chunk(m, b, q), rb.at[m, b, q], {"row": jnp.minimum(r + 1, nr - 1)}, cond)

    def to_dn(m, b, q, cond):
        send(b_chunk(m, b, q), b_chunk(m, b, q), rb.at[m, b, q], {"row": jnp.maximum(r - 1, 0)}, cond)

    def to_depth(b, q, cond=None):
        for p in peers:
            send(b_chunk(d, b, q), b_chunk(d, b, q), rb.at[d, b, q], {"depth": p}, cond)

    def a_to_col(m):
        for k in range(1, nc):
            send(abuf.at[m, c], abuf.at[m, c], ra.at[m, c], {"col": lax.rem(c + k, nc)})

    for p in peers:
        src = go_ref.at[0, :, pl.ds(pl.multiple_of(p * fh, 128), fh)]
        send(src, abuf.at[d, c], ra.at[d, c], {"depth": p})
    load_b.wait()
    for q in range(Q):
        to_up(d, r, q, has_up)
        to_dn(d, r, q, has_dn)
        to_depth(r, q)
    load_a.wait()
    a_to_col(d)

    def transpose_a(m):
        def blk(cc, _):
            def tile(j, _):
                j0 = pl.multiple_of(j * 128, 128)
                at[m, pl.ds(j0, 128), pl.ds(pl.multiple_of(cc * ta, 128), ta)] = abuf[
                    m, cc, :, pl.ds(j0, 128)
                ].T
                return 0

            return lax.fori_loop(0, fh // 128, tile, 0)

        lax.fori_loop(0, nc, blk, 0)

    tm, tn = min(512, fh), min(512, gw)

    def multiply(m, b, q0, q1, first=False):
        rows = (q1 - q0) * cb

        def tile(i, _):
            i0 = pl.multiple_of((i // (gw // tn)) * tm, tm)
            j0 = pl.multiple_of(lax.rem(i, gw // tn) * tn, tn)
            left = at[m, pl.ds(i0, tm), pl.ds(pl.multiple_of(b * tb + q0 * cb, 128), rows)]
            right = bbuf[m, b, pl.ds(q0 * cb, rows), pl.ds(j0, tn)]
            part = jnp.dot(left, right, preferred_element_type=jnp.float32)
            if first:
                acc[pl.ds(i0, tm), pl.ds(j0, tn)] = part
            else:
                acc[pl.ds(i0, tm), pl.ds(j0, tn)] += part
            return 0

        lax.fori_loop(0, (fh // tm) * (gw // tn), tile, 0)

    def both_sides(s, fn):
        def side(i, _):
            b = r + s * (2 * i - 1)

            @pl.when(jnp.logical_and(b >= 0, b < nr))
            def _():
                fn(b)

            return 0

        lax.fori_loop(0, 2, side, 0)

    def wait_a(m):
        for k in range(1, nc):
            cc = lax.rem(c + k, nc)
            arrived(abuf.at[m, cc], ra.at[m, cc])

    def forward_a():
        for p in peers:
            arrived(abuf.at[p, c], ra.at[p, c])
            a_to_col(p)

    relay_at = max(1, nr - 2)
    for s in range(1, nr):
        lo, hi = r - s, r + s
        for q in range(Q):
            pl.when(lo >= 0)(lambda: arrived(b_chunk(d, lo, q), rb.at[d, lo, q]))
            to_up(d, lo, q, jnp.logical_and(lo >= 0, has_up))
            if not (s == 1 and q < VQ):
                to_depth(lo, q, lo >= 0)
            pl.when(hi < nr)(lambda: arrived(b_chunk(d, hi, q), rb.at[d, hi, q]))
            to_dn(d, hi, q, jnp.logical_and(hi < nr, has_dn))
            if not (s == 1 and q < VQ):
                to_depth(hi, q, hi < nr)
            if s == 1 and q == (Q - 1) // 2:
                forward_a()
        if s == relay_at:
            for p in peers:
                for q in range(Q):
                    arrived(b_chunk(p, r, q), rb.at[p, r, q])
                    if q < VQ:
                        to_up(p, r, q, has_up)
                        to_dn(p, r, q, has_dn)
        if s == 1:
            wait_a(d)
            transpose_a(d)
            multiply(d, r, 0, Q, first=True)
        both_sides(s, lambda b: multiply(d, b, 0, Q))
        if s == relay_at:
            for p in peers:
                wait_a(p)
                transpose_a(p)
                multiply(p, r, 0, Q)

    def take(p, b, q0, q1):
        for q in range(q0, q1):
            arrived(b_chunk(p, b, q), rb.at[p, b, q])
        multiply(p, b, q0, q1)

    half = max(1, Q // 2)
    for s in list(range(2, nr)) + [1]:
        for p in peers:
            for q0 in range(0, Q, half):
                both_sides(s, lambda b: take(p, b, q0, q0 + half))

    def store(i, _):
        i0 = pl.multiple_of(i * 128, 128)
        out_ref[pl.ds(i0, 128), :] = acc[pl.ds(i0, 128), :].astype(out_ref.dtype)
        return 0

    lax.fori_loop(0, fh // 128, store, 0)
    for cond, copy in pending:
        if cond is None:
            copy.wait_send()
        else:
            pl.when(cond)(copy.wait_send)


def count_sends(nr, nc, nd, Q):
    return (nd - 1) + nd * (nc - 1) + 2 * nr * Q * nd + 2 * (nd - 1) * Q


MIB = 2**20


def split_kernel(
    nr, nc, J, QA, QX, go_ref, in_ref, out_ref,
    abuf, at, bbuf, acc, stage, relay, loads, ro2, rp, rc, rt, rx, rn, rf, sb, sa, single,
):
    r, c, d = lax.axis_index("row"), lax.axis_index("col"), lax.axis_index("depth")
    e = 1 - d
    core = lax.rem(c, 2)
    sib = c + 1 - 2 * core
    others = [lax.rem(c + 2 * k, nc) for k in range(1, nc // 2)]
    nd = 2
    ta, f = abuf.shape[2], abuf.shape[3]
    w = bbuf.shape[3]
    tb = bbuf.shape[2] // nr
    fh, gh = f // nd, J * w
    ca = ta // QA
    has_up, has_dn = r < nr - 1, r > 0
    up, dn = {"row": jnp.minimum(r + 1, nr - 1)}, {"row": jnp.maximum(r - 1, 0)}
    peer, twin = {"depth": e}, {"col": sib}
    groups = [(0, J // 4), (J // 4, J // 4), (J // 2, J // 2)]
    home = c // 2
    LEAD = J // 4
    sx, so, ro, sr = (single.at[k] for k in range(4))
    tail = jnp.logical_or(r == 1, r == nr - 2)
    tail_row, tail_b = jnp.where(r == 1, 0, nr - 1), jnp.where(r == 1, nr - 1, 0)

    def cols(half, j):
        return pl.ds(pl.multiple_of(half * gh + j * w, 128), w)

    def b_piece(m, b, j):
        return bbuf.at[m, j, tokens(b)]

    def tokens(b):
        return pl.ds(pl.multiple_of(b * tb, 128), tb)

    def a_piece(m, cc, q):
        return abuf.at[m, cc, pl.ds(q * ca, ca)]

    def loop(n, fn, unroll=1):
        lax.fori_loop(0, n, lambda i, _: (fn(i), 0)[1], 0, unroll=unroll)

    def arrived(ref, sem):
        pltpu.make_async_copy(ref, ref, sem).wait()

    def send(src, dst, send_sem, recv_sem, device):
        pltpu.make_async_remote_copy(
            src_ref=src, dst_ref=dst, send_sem=send_sem, recv_sem=recv_sem,
            device_id=device, device_id_type=MESH,
        ).start()

    barrier = pltpu.get_barrier_semaphore()

    def greet(device):
        pl.semaphore_signal(barrier, inc=1, device_id=device, device_id_type=MESH)

    pl.when(has_up)(lambda: greet(up))
    pl.when(has_dn)(lambda: greet(dn))
    greet(peer)
    greet(twin)
    for o in others:
        greet({"col": o})
    at_end = jnp.logical_not(jnp.logical_and(has_up, has_dn))

    @pl.when(jnp.logical_and(at_end, core == 0))
    def _():
        greet({"row": jnp.where(r == 0, 1, nr - 2), "col": sib})

    loop(J, lambda j: pltpu.make_async_copy(in_ref.at[0, :, cols(d, j)], b_piece(d, r, j), loads.at[0]).start())
    load_a = pltpu.make_async_copy(go_ref.at[0], abuf.at[d, c], loads.at[1])
    load_a.start()

    pl.semaphore_wait(
        barrier,
        2 + len(others) + jnp.where(has_up, 1, 0) + jnp.where(has_dn, 1, 0)
        + jnp.where(jnp.logical_and(tail, core == 1), 1, 0),
    )

    def b_send(way, m, b, j, recv_sem):
        send(b_piece(m, b, j), b_piece(m, b, j), sb.at[way, b], recv_sem, (up, dn)[way])

    def b_both(k, g):
        m = (d, e)[k]

        def one(i):
            j = groups[g][0] + i
            pl.when(has_up)(lambda: b_send(0, m, r, j, rn.at[0, k, min(g, 1)]))
            pl.when(has_dn)(lambda: b_send(1, m, r, j, rn.at[1, k, min(g, 1)]))

        loop(groups[g][1], one)

    def group_wait(g):
        arrived(bbuf.at[e, pl.ds(*groups[g]), tokens(r)], rx.at[g])

    def near_wait(k, b, side, g):
        span = pl.ds(0, LEAD) if g == 0 else pl.ds(LEAD, J - LEAD)
        arrived(bbuf.at[(d, e)[k], span, tokens(b)], rn.at[side, k, g])

    def far_slot(b, row):
        return jnp.where(b < row, b, b - 2 - jnp.where(row > 0, 1, 0))

    def far_sem(k, b, j, row):
        return rf.at[far_slot(b, row), j + k * jnp.where(j == J - 1, 1, 0)]

    def far_wait(k, b, j):
        m = jnp.where(k == 0, d, e)
        pl.when(jnp.logical_and(k == 0, j < J - 1))(lambda: arrived(bbuf.at[:, j, tokens(b)], rf.at[far_slot(b, r), j]))
        pl.when(j == J - 1)(lambda: arrived(b_piece(m, b, j), far_sem(k, b, j, r)))

    def corner_sem(o, q):
        return rc.at[o // 2, q // 2 + jnp.where(q == QA - 1, 1, 0)]

    def a_send(kind, m, cc, q, device, recv_sem):
        send(a_piece(m, cc, q), a_piece(m, cc, q), sa.at[kind], recv_sem, device)

    def a_twin(m, cc, q, away=0):
        a_send(0, m, cc, q, twin, rt.at[m, away])

    def group_of(j):
        return sum(jnp.where(j >= groups[g][0], 1, 0) for g in range(1, len(groups)))

    arrived(bbuf.at[d, :, tokens(r)], loads.at[0])
    b_both(0, 0)
    loop(J, lambda j: send(in_ref.at[0, :, cols(e, j)], b_piece(d, r, j), sx, rx.at[group_of(j)], peer))
    for g in range(1, len(groups)):
        b_both(0, g)
    load_a.wait()

    def own_a(q):
        a_send(1, d, c, q, peer, rp.at[q])
        for k, o in enumerate(others):
            a_send(3 + 2 * k, d, c, q, {"col": o}, ro2.at[home, q // 2])
        a_twin(d, c, q)

    loop(QA, own_a)
    group_wait(0)
    b_both(1, 0)
    for g in range(1, len(groups)):
        group_wait(g)
        b_both(1, g)

    def pass_near(j):
        for k, m in enumerate((d, e)):
            pl.when(jnp.logical_and(r >= 1, has_up))(lambda: b_send(0, m, r - 1, j, far_sem(k, r - 1, j, r + 1)))
            pl.when(jnp.logical_and(r + 1 < nr, has_dn))(lambda: b_send(1, m, r + 1, j, far_sem(k, r + 1, j, r - 1)))

    def wait_near(k, g, passed):
        for side, b, ok, way in ((0, r - 1, r >= 1, has_up), (1, r + 1, r + 1 < nr, has_dn)):
            way = way if passed else jnp.logical_not(way)
            pl.when(jnp.logical_and(ok, way))(lambda: near_wait(k, b, side, g))

    def pass_far(s, j):
        lo, hi = r - s, r + s
        def go(way, k, b):
            m = (d, e)[k]
            far_wait(k, b, j)
            if s < nr - 2:
                return b_send(way, m, b, j, far_sem(k, b, j, (r + 1, r - 1)[way]))
            aside = jnp.logical_and(j == J - 1, core == 0)
            pl.when(jnp.logical_not(aside))(lambda: b_send(way, m, b, j, far_sem(k, b, j, (r + 1, r - 1)[way])))
            pl.when(aside)(lambda: send(b_piece(m, b, j), relay.at[k], sr, single.at[4 + k], twin))

        for k in range(2):
            pl.when(jnp.logical_and(lo >= 0, has_up))(lambda: go(0, k, lo))
            pl.when(jnp.logical_and(hi < nr, has_dn))(lambda: go(1, k, hi))

    def pass_relay():
        @pl.when(tail)
        def _():
            for k, m in enumerate((d, e)):
                arrived(relay.at[k], single.at[4 + k])
                send(relay.at[k], b_piece(m, tail_b, J - 1), sr, far_sem(k, tail_b, J - 1, tail_row), {"row": tail_row, "col": sib})

    def near(j):
        pl.when(j < J)(lambda: pass_near(j))

    def far(j):
        @pl.when(j < J)
        def _():
            for s in range(2, nr):
                pass_far(s, j)

    def pair_wait(m, cc, q, sem):
        arrived(abuf.at[m, cc, pl.ds(q * ca, 2 * ca)], sem)

    def from_other(q):
        for o in others:
            if q % 2 == 0:
                pair_wait(d, o, q, ro2.at[o // 2, q // 2])
            a_twin(d, o, q, 1)
            if q < QX:
                a_send(2, d, o, q, peer, corner_sem(o, q))

    def from_peer(q):
        arrived(a_piece(e, c, q), rp.at[q])
        if not isinstance(q, int) or q >= QX:
            for k, o in enumerate(others):
                a_send(4 + 2 * k, e, c, q, {"col": o}, corner_sem(c, q))
        a_twin(e, c, q)

    def from_corner(q):
        for o in others:
            @pl.when(q >= QA - 2)
            def _():
                arrived(a_piece(e, o, q), corner_sem(o, q))
                a_twin(e, o, q, 1)

            @pl.when(jnp.logical_and(q < QA - 2, lax.rem(q, 2) == 1))
            def _():
                pair_wait(e, o, q - 1, corner_sem(o, q))
                a_twin(e, o, q - 1, 1)
                a_twin(e, o, q, 1)

    def from_twin(m, away):
        arrived(abuf.at[m, pl.ds(0, len(others) if away else 1)], rt.at[m, away])

    def transpose_a(m, away):
        def blk(i):
            cc = lax.rem(2 * home + 2 * away + i, nc)

            def tile(j):
                j0 = pl.multiple_of(j * 128, 128)
                at[m, pl.ds(j0, 128), pl.ds(pl.multiple_of(cc * ta, 128), ta)] = abuf[
                    m, cc, :, pl.ds(j0, 128)
                ].T

            loop(f // 128, tile, unroll=4)

        loop(nc - 2 if away else 2, blk)

    tm = min(512, fh)

    def left(m, b, i):
        return at[m, pl.ds(i * tm, tm), tokens(b)]

    def multiply_pair(m, b, p):
        j = 2 * p
        right = jnp.concatenate([b_piece(m, b, j)[...], b_piece(m, b, j + 1)[...]], axis=1)
        for i in range(f // tm):
            rows = pl.ds(i * tm, tm)
            part = jnp.dot(left(m, b, i), right, preferred_element_type=jnp.float32)
            for k in range(2):
                acc[j + k, rows] += part[:, k * w : (k + 1) * w]

    def multiply(m, b, j):
        right = b_piece(m, b, j)[...]
        for i in range(f // tm):
            rows = pl.ds(i * tm, tm)
            acc[j, rows] += jnp.dot(left(m, b, i), right, preferred_element_type=jnp.float32)

    def not_passed(b):
        return jnp.logical_or(
            jnp.logical_and(b < r, jnp.logical_not(has_up)),
            jnp.logical_and(b > r, jnp.logical_not(has_dn)),
        )

    def at_home(b):
        return b // 2 == home

    def near_blocks(fn, cond=None):
        def one(i):
            b = r - 1 + i
            ok = jnp.logical_and(b >= 0, b < nr)
            pl.when(ok if cond is None else jnp.logical_and(ok, cond(b)))(lambda: fn(b))

        loop(3, one)

    def clear(i):
        acc[i // 4, pl.ds(pl.multiple_of(lax.rem(i, 4) * (f // 4), 128), f // 4)] = jnp.zeros((f // 4, w), jnp.float32)

    loop(4 * J, clear)
    wait_near(0, 0, True)
    wait_near(1, 0, True)
    loop(LEAD, near)
    from_twin(d, 0)
    transpose_a(d, 0)
    half = QA // 2
    for q in range(half):
        from_other(q)
    for q in range(half):
        from_other(half + q)
        from_peer(q)
    wait_near(0, 1, True)
    wait_near(1, 1, True)
    for g in range(2):
        wait_near(0, g, False)
    from_twin(d, 1)
    transpose_a(d, 1)

    def step(t):
        far(t)
        pl.when(t + 1 >= LEAD)(lambda: near(t + 1))

    def first_near(i):
        b = r - 1 + i
        pl.when(jnp.logical_and(b >= 0, b < nr))(lambda: loop(J // 2, lambda p: multiply_pair(d, b, p)))
        from_peer(half + i)
        from_corner(QX + i)
        step(i)

    loop(3, first_near)
    for q in range(half + 3, QA):
        from_peer(q)
        from_corner(q - half + QX)
    step(3)
    from_twin(e, 0)
    for g in range(2):
        wait_near(1, g, False)
    transpose_a(e, 0)
    near_blocks(lambda b: loop(J // 2, lambda p: multiply_pair(e, b, p)), at_home)

    def far_blocks(fn):
        def one(i):
            s, b = 2 + i // 2, r + (2 + i // 2) * (2 * lax.rem(i, 2) - 1)
            pl.when(jnp.logical_and(b >= 0, b < nr))(lambda: fn(s, b))

        loop(2 * (nr - 2), one)

    def early(j):
        def one(s, b):
            pl.when(not_passed(b))(lambda: far_wait(0, b, j))

            def part(k):
                pl.when(jnp.logical_or(k == 0, at_home(b)))(lambda: multiply(jnp.where(k == 0, d, e), b, j))

            loop(2, part)

        far_blocks(one)

    for q in range(QA - half + QX, QA - 1):
        from_corner(q)
    for q in range(QX - 1):
        from_corner(q)
    step(4)
    early(0)
    from_corner(QA - 1)
    from_corner(QX - 1)
    early(1)
    from_twin(e, 1)
    transpose_a(e, 1)

    def away(b):
        return jnp.logical_not(at_home(b))

    span = jnp.logical_or(r == 0, r == nr - 1)
    end_b = jnp.where(r == 0, nr - 1, 0)
    hh = fh // 4

    def settle_sends():
        arrived(bbuf.at[d, :, tokens(r)], sx)
        arrived(abuf.at[:, pl.ds(0, nc // 2)], sa.at[0])
        arrived(abuf.at[d, c], sa.at[1])
        arrived(abuf.at[d, pl.ds(0, len(others)), pl.ds(0, QX * ca)], sa.at[2])
        for k in range(len(others)):
            arrived(abuf.at[d, c], sa.at[3 + 2 * k])
            arrived(abuf.at[d, c, pl.ds(0, (QA - QX) * ca)], sa.at[4 + 2 * k])
        pl.when(has_up)(lambda: arrived(bbuf.at[:, :, tokens(r)], sb.at[0, r]))
        pl.when(has_dn)(lambda: arrived(bbuf.at[:, :, tokens(r)], sb.at[1, r]))

    def column(j):
        t = j + 4
        pl.when(jnp.logical_and(t > 4, t < J - 1))(lambda: far(t))
        pl.when(jnp.logical_and(t > 4, t < J - 2))(lambda: near(t + 1))

        @pl.when(t == J - 1 + core)
        def _():
            pl.when(core == 1)(pass_relay)
            near(J - 1)
            far(J - 1)

        def block(s, b):
            def part(k):
                todo = jnp.logical_or(j >= 2, jnp.logical_and(k == 1, away(b)))
                todo = jnp.logical_and(todo, jnp.logical_or(s < nr - 1, k == 0))

                @pl.when(todo)
                def _():
                    pl.when(jnp.logical_and(j >= 2, not_passed(b)))(lambda: far_wait(k, b, j))
                    multiply(jnp.where(k == 0, d, e), b, j)

            loop(2, part)

        far_blocks(block)
        pl.when(j == J - 1)(settle_sends)
        left_over = jnp.logical_and(span, jnp.logical_or(j >= 2, away(end_b)))
        pl.when(jnp.logical_and(left_over, j >= 2))(lambda: far_wait(1, end_b, j))

        def leave(i):
            rows = pl.ds(pl.multiple_of(i * hh, 128), hh)
            send(stage.at[j, rows], out_ref.at[rows, cols(d, j)], so, ro, peer)

        def quarter(i):
            rows = pl.ds(pl.multiple_of(jnp.where(i < 4, e, d) * fh + lax.rem(i, 4) * hh, 128), hh)

            @pl.when(left_over)
            def _():
                acc[j, rows] += jnp.dot(
                    at[e, rows, tokens(end_b)], b_piece(e, end_b, j)[...], preferred_element_type=jnp.float32
                )

            here = pl.ds(pl.multiple_of(lax.rem(i, 4) * hh, 128), hh)
            done = acc[j, rows].astype(jnp.bfloat16)

            @pl.when(i < 4)
            def _():
                stage[j, here] = done

            @pl.when(i >= 4)
            def _():
                out_ref[here, cols(d, j)] = done

            pl.when(jnp.logical_and(i >= 1, i < 5))(lambda: leave(i - 1))

        loop(8, quarter)

    def pair(p):
        near_blocks(lambda b: multiply_pair(e, b, p), away)
        loop(2, lambda k: column(2 * p + k))

    loop(J // 2, pair)

    def drain(b):
        short = jnp.logical_and(jnp.logical_and(tail, core == 0), b == tail_b)
        full = jnp.logical_not(jnp.logical_or(short, b == r))
        for way, ok in enumerate((jnp.logical_and(has_up, b <= r), jnp.logical_and(has_dn, b >= r))):
            pl.when(jnp.logical_and(ok, full))(lambda: arrived(bbuf.at[:, :, tokens(b)], sb.at[way, b]))
            pl.when(jnp.logical_and(ok, short))(lambda: arrived(bbuf.at[:, pl.ds(0, J - 1), tokens(b)], sb.at[way, b]))

    loop(nr, drain)
    pl.when(tail)(lambda: arrived(relay, sr))
    arrived(stage, so)
    arrived(out_ref.at[:, pl.ds(pl.multiple_of(e * gh, 128), gh)], ro)


def split_plan(nr, nc, nd, ta, tb, f, gw):
    w = 128
    if nd != 2 or nc % 2 or nc < 4 or nr < 4 or nr != nc or ta != tb or gw % (nd * 8 * w) or ta % 512 or tb % 128 or f % 1024:
        return None
    J = gw // (nd * w)
    shapes = [
        ((nd, nc, ta, f), jnp.bfloat16),
        ((nd, f, ta * nc), jnp.bfloat16),
        ((nd, J, tb * nr, w), jnp.bfloat16),
        ((J, f, w), jnp.float32),
        ((J, f // nd, w), jnp.bfloat16),
        ((2, tb, w), jnp.bfloat16),
    ]
    size = sum(math.prod(s) * jnp.dtype(t).itemsize for s, t in shapes)
    return (J, shapes) if size <= 52 * MIB else None


def split_body(nr, nc, nd, plan, grad_out, inputs):
    J, shapes = plan
    _, ta, f = grad_out.shape
    gw = inputs.shape[2]
    QA, QX = 8, 2
    return pl.pallas_call(
        functools.partial(split_kernel, nr, nc, J, QA, QX),
        out_shape=pltpu.VMEM((f // nd, gw), jnp.bfloat16),
        in_specs=[pl.BlockSpec(memory_space=pl.ANY)] * 2,
        out_specs=pl.BlockSpec(memory_space=pltpu.VMEM),
        scratch_shapes=[pltpu.VMEM(s, t) for s, t in shapes] + [
            pltpu.SemaphoreType.DMA((2,)),
            pltpu.SemaphoreType.DMA((nc // 2, QA // 2)),
            pltpu.SemaphoreType.DMA((QA,)),
            pltpu.SemaphoreType.DMA((nc // 2, QA // 2 + 1)),
            pltpu.SemaphoreType.DMA((nd, 2)),
            pltpu.SemaphoreType.DMA((3,)),
            pltpu.SemaphoreType.DMA((2, 2, 2)),
            pltpu.SemaphoreType.DMA((nr - 2, J + 1)),
            pltpu.SemaphoreType.DMA((2, nr)),
            pltpu.SemaphoreType.DMA((1 + nc,)),
            pltpu.SemaphoreType.DMA((6,)),
        ],
        compiler_params=pltpu.CompilerParams(
            collective_id=1, has_side_effects=True, vmem_limit_bytes=58 * MIB
        ),
    )(grad_out, inputs)


def body(nr, nc, nd, grad_out, inputs):
    _, ta, f = grad_out.shape
    _, tb, gw = inputs.shape
    fh = f // nd
    Q = max(1, min(4, 32 // (nd * nr)))
    VQ = 3 * Q // 4
    tokens = tb * nr
    plan = split_plan(nr, nc, nd, ta, tb, f, gw)
    if plan is not None:
        return split_body(nr, nc, nd, plan, grad_out, inputs)
    return pl.pallas_call(
        functools.partial(kernel, nr, nc, nd, Q, VQ),
        out_shape=pltpu.VMEM((fh, gw), jnp.bfloat16),
        in_specs=[pl.BlockSpec(memory_space=pl.ANY)] * 2,
        out_specs=pl.BlockSpec(memory_space=pltpu.VMEM),
        scratch_shapes=[
            pltpu.VMEM((nd, nc, ta, fh), jnp.bfloat16),
            pltpu.VMEM((nd, fh, tokens), jnp.bfloat16),
            pltpu.VMEM((nd, nr, tb, gw), jnp.bfloat16),
            pltpu.VMEM((fh, gw), jnp.float32),
            pltpu.SemaphoreType.DMA((2,)),
            pltpu.SemaphoreType.DMA((nd, nc)),
            pltpu.SemaphoreType.DMA((nd, nr, Q)),
            pltpu.SemaphoreType.DMA((count_sends(nr, nc, nd, Q),)),
        ],
        compiler_params=pltpu.CompilerParams(
            collective_id=0, has_side_effects=True, vmem_limit_bytes=52 * 2**20
        ),
    )(grad_out, inputs)


def solution(mesh):
    return jax.shard_map(
        functools.partial(body, mesh.shape["row"], mesh.shape["col"], mesh.shape["depth"]),
        mesh=mesh,
        in_specs=(P("depth", "col", "row"), P("depth", "row", "col")),
        out_specs=P(("row", "depth"), "col"),
        check_vma=False,
    )
```
